128 devices in a mesh: tm: 16 (over x, y), series: 8 (over z, core).
Axes of the slice: x: 4, y: 4, z: 4, core: 2. Of those that a mesh axis runs over, the one named last changes fastest.
Arguments:
- tokens: bfloat16 [16, 8192, 1024], P('series', 'tm'), may hold values from -6 to 6
- gate_proj: bfloat16 [1024, 2048], replicated, may hold values from -0.1875 to 0.1875
- input_proj: bfloat16 [1024, 2304], replicated, may hold values from -0.1875 to 0.1875
- step_proj: bfloat16 [1024, 32], replicated, may hold values from -0.1875 to 0.1875
- conv_kernel: float32 [4, 2304], replicated, may hold values from -3 to 3
- conv_bias: float32 [2304], replicated, may hold values from -0.5 to 0.5
- step_bias: float32 [32], replicated, may hold values from -1 to 1
- decay_rate: float32 [32], replicated, may hold values from 6.1035156e-05 to 0.1
- skip_gain: float32 [32], replicated, may hold values from 0.5 to 1.5
- norm_gain: float32 [2048], replicated, may hold values from 0.1 to 1.9
- out_proj: bfloat16 [2048, 1024], replicated, may hold values from -0.125 to 0.125
- lengths: int32 [16], P('series'), may hold values from 256 to 8192, as said below
- slot_series: int32 [16], P('series'), may hold values from 0 to 15, each once
Outputs:
- mixed: bfloat16 [16, 8192, 1024], P('series', 'tm')
The draws below stay inside these ranges and needn't reach their ends.
Inputs may be any that keep to these rules, and one draw needn't show every extreme that they name: `lengths`: multiples of 256; some series has the full 8192. `slot_series`: each series number appears once.
All inputs are finite; a program needn't handle non-finite values.
Results may differ from the reference program's by a relative error of at most 0.0054.
Values may be sent and summed in bfloat16 or wider, within the bound.
A program may use at most 128 MiB of HBM per device.

```python
import math
import jax
import jax.numpy as jnp
from jax import lax

D = 1024
DI = 2048
H = 32
P_SIZE = 64
N = 128
KERNEL = 4
BLOCK = 256
SERIES = 16
STEPS = 8192


def draw_lengths(key, part):
    blocks_total = STEPS // BLOCK
    counts = jax.random.randint(jax.random.fold_in(key, 11), (SERIES,), 1, blocks_total + 1)
    full_one = jax.random.randint(jax.random.fold_in(key, 12), (), 0, SERIES)
    counts = jnp.where(jnp.arange(SERIES) == full_one, blocks_total, counts)
    return (counts * BLOCK).astype(jnp.int32)


def block_levels(rng, extent, cuts, least, largest):
    level, own = 1.0, jax.random.fold_in(rng, 6)
    for dim, shards_of in cuts:
        steps = jnp.exp(jax.random.uniform(jax.random.fold_in(own, dim), (shards_of,), jnp.float32, least / len(cuts), largest / len(cuts)))
        level = level * jnp.repeat(steps, extent[dim] // shards_of).reshape([-1 if axis == dim else 1 for axis in range(len(extent))])
    return level


def scatter_about(rng, shape, scale, reach, split=(), held_as=jnp.bfloat16):
    entries = scale * jax.random.normal(rng, shape, jnp.float32)
    if split:
        entries = entries * block_levels(rng, shape, split, -0.22, 0.18)
    return jnp.clip(entries, -reach, reach).astype(held_as)


def setup_inputs(seed: int = 0) -> dict:
    splits = jax.random.split(jax.random.key(seed), 14)
    return {
        "tokens": scatter_about(splits[0], (SERIES, STEPS, D), 1.0, 6.0, ((0, 8), (1, 16))),
        "gate_proj": scatter_about(splits[1], (D, DI), D ** -0.5, 0.1875),
        "input_proj": scatter_about(splits[2], (D, DI + 2 * N), D ** -0.5, 0.1875),
        "step_proj": scatter_about(splits[3], (D, H), D ** -0.5, 0.1875),
        "conv_kernel": scatter_about(splits[4], (KERNEL, DI + 2 * N), 0.5, 3.0, (), jnp.float32),
        "conv_bias": jnp.clip(jax.random.uniform(splits[5], (DI + 2 * N,), jnp.float32, -0.5, 0.5), -0.5, 0.5),
        "step_bias": jnp.clip(jax.random.uniform(splits[6], (H,), jnp.float32, -1.0, 1.0), -1.0, 1.0),
        "decay_rate": jnp.clip(jnp.exp(jax.random.uniform(splits[7], (H,), jnp.float32, math.log(6.103515625e-05), math.log(0.1))), 6.103515625e-05, 0.1),
        "skip_gain": jnp.clip(jax.random.uniform(splits[8], (H,), jnp.float32, 0.5, 1.5), 0.5, 1.5),
        "norm_gain": jnp.clip(1.0 + 0.18 * jax.random.normal(splits[9], (DI,), jnp.float32), 0.1, 1.9),
        "out_proj": scatter_about(splits[10], (DI, D), DI ** -0.5, 0.125),
        "lengths": draw_lengths(jax.random.fold_in(splits[13], 71), 0),
        "slot_series": jax.random.permutation(splits[12], SERIES).astype(jnp.int32),
    }


epsilon = 1e-05

def block_terms(inputs_x, inputs_b, inputs_c, step_sizes, decay_rate, skip_gain):
    width_q = inputs_x.shape[0]
    cumulative = jnp.cumsum(-step_sizes * decay_rate[None, :], axis=0)
    heads_cum = cumulative.T
    causal = jnp.tril(jnp.ones((width_q, width_q), dtype=bool))[None]
    segment = heads_cum[:, :, None] - heads_cum[:, None, :]
    decays = jnp.where(causal, jnp.exp(jnp.where(causal, segment, 0.0)), 0.0)
    scores = jnp.dot(inputs_c, inputs_b.T, preferred_element_type=jnp.float32)
    weights = (decays * scores[None] * step_sizes.T[:, None, :]).astype(jnp.bfloat16)
    intra = jnp.einsum('hts,shp->thp', weights.astype(jnp.float32), inputs_x.astype(jnp.float32))
    partial_out = intra + skip_gain[None, :, None] * inputs_x.astype(jnp.float32)
    end_weight = jnp.exp(cumulative[-1][None, :] - cumulative) * step_sizes
    weighted_x = (inputs_x.astype(jnp.float32) * end_weight[:, :, None]).astype(jnp.bfloat16)
    increment = jnp.einsum('shp,sn->hpn', weighted_x.astype(jnp.float32), inputs_b.astype(jnp.float32))
    return (partial_out, cumulative, increment)

def reference(tokens, gate_proj, input_proj, step_proj, conv_kernel, conv_bias, step_bias, decay_rate, skip_gain, norm_gain, out_proj, lengths, slot_series):
    series_lengths = lengths[slot_series]

    def one_series(pair):
        row_tokens, length_now = pair
        total_steps = row_tokens.shape[0]
        gate = jnp.dot(row_tokens, gate_proj, preferred_element_type=jnp.float32)
        mixed_raw = jnp.dot(row_tokens, input_proj, preferred_element_type=jnp.float32).astype(jnp.bfloat16)
        step_raw = jnp.dot(row_tokens, step_proj, preferred_element_type=jnp.float32)
        kernel_len = conv_kernel.shape[0]
        padded = jnp.concatenate([jnp.zeros((kernel_len - 1, mixed_raw.shape[1]), jnp.bfloat16), mixed_raw], axis=0)
        convolved = jnp.zeros(mixed_raw.shape, jnp.float32) + conv_bias[None, :]
        for offset in range(kernel_len):
            convolved = convolved + conv_kernel[offset][None, :] * padded[offset:offset + total_steps].astype(jnp.float32)
        activated = jax.nn.silu(convolved)
        block_count = total_steps // BLOCK
        inputs_x = activated[:, :DI].astype(jnp.bfloat16).reshape(block_count, BLOCK, H, P_SIZE)
        inputs_b = activated[:, DI:DI + N].astype(jnp.bfloat16).reshape(block_count, BLOCK, N)
        inputs_c = activated[:, DI + N:].astype(jnp.bfloat16).reshape(block_count, BLOCK, N)
        live = (jnp.arange(total_steps, dtype=jnp.int32) < length_now).astype(jnp.float32)
        step_sizes = (jax.nn.softplus(step_raw + step_bias[None, :]) * live[:, None]).reshape(block_count, BLOCK, H)

        def advance(state, pieces):
            block_x, block_b, block_c, block_dt = pieces
            partial_out, cumulative, increment = block_terms(block_x, block_b, block_c, block_dt, decay_rate, skip_gain)
            state_bf = state.astype(jnp.bfloat16)
            inter = jnp.einsum('tn,hpn->thp', block_c.astype(jnp.float32), state_bf.astype(jnp.float32))
            output = partial_out + jnp.exp(cumulative)[:, :, None] * inter
            state = jnp.exp(cumulative[-1])[:, None, None] * state + increment
            return (state, output)
        start_state = jnp.zeros((H, P_SIZE, N), jnp.float32)
        ignored, outputs = lax.scan(advance, start_state, (inputs_x, inputs_b, inputs_c, step_sizes))
        outputs = outputs.reshape(total_steps, DI)
        gated = outputs * jax.nn.silu(gate)
        scale = lax.rsqrt(lax.optimization_barrier(jnp.mean(gated * gated, axis=1, keepdims=True)) + epsilon)
        normed = (gated * scale * norm_gain[None, :]).astype(jnp.bfloat16)
        result = jnp.dot(normed, out_proj, preferred_element_type=jnp.float32) * live[:, None]
        return result.astype(jnp.bfloat16)
    return lax.map(one_series, (tokens, series_lengths))
```

```python
import functools

import jax
import jax.numpy as jnp
from jax import lax
from jax.experimental import pallas as pl
from jax.experimental.pallas import tpu as pltpu
from jax.sharding import PartitionSpec as P

MESH = pl.DeviceIdType.MESH
F32 = jnp.float32
BF16 = jnp.bfloat16

D = 1024
DI = 2048
H = 32
N = 128
KT = 4
W_IN = DI + 2 * N
Q = 128
EPS = 1e-05
LOG2E = 1.4426950408889634
RIM = 16
GROUPS = 4
GC = DI // GROUPS


def dot(a, b, **kw):
    return jnp.dot(a, b, preferred_element_type=F32, **kw)


def hilo(v):
    hi = v.astype(BF16)
    lo = (v - hi.astype(F32)).astype(BF16)
    return jnp.concatenate([hi, lo], axis=1)


def kernel(
    n_tm,
    n_ser,
    series_here,
    steps,
    tokens_hbm,
    gate_hbm,
    in_hbm,
    stepw_ref,
    convk_ref,
    convb_ref,
    stepb_ref,
    rate_ref,
    skip_ref,
    gain_ref,
    out_w_hbm,
    len_smem,
    slot_smem,
    out_hbm,
    tok,
    win,
    wgate,
    wout,
    xs,
    bt,
    raw,
    cumc,
    crt,
    fhl,
    ghl,
    eh,
    rows,
    rowx,
    sl,
    scur,
    sin,
    yb,
    sg,
    nb,
    isend,
    irecv,
    ssend,
    srecv,
    dsend,
    drecv,
    dxs,
    lsend,
    lrecv,
    lenv,
    load_sem,
    out_sem,
    len_ssem,
    len_rsem,
    rim_ssem,
    rim_rsem,
    d_ssem,
    d_rsem,
    i_ssem,
    i_rsem,
    s_ssem,
    s_rsem,
):
    me = lax.axis_index("tm")
    ser = lax.axis_index("series")
    chunks = steps // Q
    nc = series_here * chunks

    loads = []
    for s in range(series_here):
        loads.append(
            pltpu.make_async_copy(
                tokens_hbm.at[s], tok.at[s, pl.ds(RIM, steps), :], load_sem.at[s]
            )
        )
    loads.append(pltpu.make_async_copy(in_hbm, win, load_sem.at[2]))
    loads.append(pltpu.make_async_copy(gate_hbm, wgate, load_sem.at[3]))
    loads.append(pltpu.make_async_copy(out_w_hbm, wout, load_sem.at[4]))
    for c in loads:
        c.start()

    barrier = pltpu.get_barrier_semaphore()

    def greet_tm(k, carry):
        @pl.when(k != me)
        def _():
            pl.semaphore_signal(barrier, inc=1, device_id=(k, ser), device_id_type=MESH)

        return carry

    def greet_ser(k, carry):
        @pl.when(k != ser)
        def _():
            pl.semaphore_signal(barrier, inc=1, device_id=(me, k), device_id_type=MESH)

        return carry

    lax.fori_loop(0, n_tm, greet_tm, 0)
    lax.fori_loop(0, n_ser, greet_ser, 0)

    lane = lax.broadcasted_iota(jnp.int32, (8, 128), 1)
    lsend[...] = jnp.where(lane == 0, len_smem[0], jnp.where(lane == 1, len_smem[1], 0))
    er = lax.broadcasted_iota(jnp.int32, (2 * H, DI), 0)
    ec = lax.broadcasted_iota(jnp.int32, (2 * H, DI), 1)
    eh[...] = jnp.where((er % H) == ec // (DI // H), 1.0, 0.0).astype(BF16)
    dsend[...] = jnp.zeros_like(dsend)
    rows[...] = jnp.zeros_like(rows)

    pl.semaphore_wait(barrier, n_tm + n_ser - 2)

    def len_copy(k, slot):
        return pltpu.make_async_remote_copy(
            src_ref=lsend,
            dst_ref=lrecv.at[slot],
            send_sem=len_ssem.at[k],
            recv_sem=len_rsem.at[slot],
            device_id=(me, k),
            device_id_type=MESH,
        )

    def send_len(k, carry):
        @pl.when(k != ser)
        def _():
            len_copy(k, ser).start()

        return carry

    lax.fori_loop(0, n_ser, send_len, 0)
    lrecv[ser] = lsend[...]

    def rim_copy(s):
        return pltpu.make_async_remote_copy(
            src_ref=tokens_hbm.at[s, pl.ds(steps - RIM, RIM), :],
            dst_ref=tok.at[s, pl.ds(0, RIM), :],
            send_sem=rim_ssem.at[s],
            recv_sem=rim_rsem.at[s],
            device_id=(lax.rem(me + 1, n_tm), ser),
            device_id_type=MESH,
        )

    @pl.when(me < n_tm - 1)
    def _():
        for s in range(series_here):
            rim_copy(s).start()

    @pl.when(me == 0)
    def _():
        for s in range(series_here):
            tok[s, 0:RIM, :] = jnp.zeros((RIM, D), BF16)

    def wait_len(k, carry):
        @pl.when(k != ser)
        def _():
            len_copy(k, k).wait_recv()

        return carry

    lax.fori_loop(0, n_ser, wait_len, 0)
    for s in range(series_here):
        sid = slot_smem[s]
        found = jnp.zeros((8, 128), jnp.int32)
        for p in range(n_ser):
            hit = (lane < series_here) & (lane + series_here * p == sid)
            found = found + jnp.where(hit, lrecv[p], 0)
        lenv[s] = jnp.broadcast_to(
            jnp.sum(found.astype(F32), axis=1, keepdims=True), (8, 128)
        )

    for s in range(series_here):
        loads[s].wait()

    tri_r = lax.broadcasted_iota(jnp.int32, (Q, Q), 0)
    tri_c = lax.broadcasted_iota(jnp.int32, (Q, Q), 1)
    neg_rate = rate_ref[...].reshape(1, H) * (-LOG2E)
    step_bias = stepb_ref[...].reshape(1, H)

    def steps_body(ci, carry):
        s = ci // chunks
        c = ci % chunks
        t0 = pl.multiple_of(RIM + c * Q, 16)
        pre = dot(tok[s, pl.ds(t0, Q), :], stepw_ref[...]) + step_bias
        first = (me * steps + c * Q).astype(F32)
        live = jnp.where(lenv[s] > first, 1.0, 0.0)
        dt = jnp.maximum(pre, 0.0) + jnp.log1p(jnp.exp(-jnp.abs(pre)))
        dt = dt * live[0:1, 0:H]
        ltri = jnp.where(tri_r >= tri_c, 1.0, 0.0)
        cum = dot(ltri, dt * neg_rate, precision=lax.Precision.HIGHEST)
        lg = jnp.where(dt > 0.0, jnp.log(jnp.where(dt > 0.0, dt, 1.0)) * LOG2E, -1e30)
        crp = cum - lg
        last = cum[Q - 1 : Q, :]
        cumc[ci] = cum
        fhl[ci] = hilo(jnp.exp2(last - crp))
        ghl[ci] = hilo(jnp.exp2(cum))
        wide = jnp.concatenate([crp, jnp.zeros((Q, 128 - H), F32)], axis=1)
        crt[ci] = wide.T[0:H, :]
        return carry

    lax.fori_loop(0, nc, steps_body, 0)

    r8 = lax.broadcasted_iota(jnp.int32, (8, H), 0)
    ecl = jnp.zeros((8, H), F32)
    ebef = jnp.zeros((8, H), F32)
    dtot = jnp.zeros((8, H), F32)
    for s in range(series_here):
        before = jnp.zeros((1, H), F32)
        for c in range(chunks):
            ci = s * chunks + c
            last = cumc[ci, Q - 1 : Q, :]
            ecl = jnp.where(r8 == ci, jnp.exp2(last), ecl)
            ebef = jnp.where(r8 == ci, jnp.exp2(before), ebef)
            before = before + last
        dtot = jnp.where(r8 == s, before, dtot)
    dsend[:, 0:H] = dtot
    rows[0:8, :] = ecl
    rows[8:16, :] = ebef
    rows[16:24, :] = jnp.broadcast_to(skip_ref[...].reshape(1, H), (8, H))
    rowx[...] = dot(hilo(rows[...]), eh[...])

    def d_copy(k, slot):
        return pltpu.make_async_remote_copy(
            src_ref=dsend,
            dst_ref=drecv.at[slot],
            send_sem=d_ssem.at[k],
            recv_sem=d_rsem.at[slot],
            device_id=(k, ser),
            device_id_type=MESH,
        )

    def send_d(k, carry):
        @pl.when(k != me)
        def _():
            d_copy(k, me).start()

        return carry

    lax.fori_loop(0, n_tm, send_d, 0)
    drecv[me] = dsend[...]

    @pl.when(me > 0)
    def _():
        for s in range(series_here):
            rim_copy(s).wait_recv()

    loads[2].wait()

    def produce(col0, width, s):
        cols = pl.ds(col0, width)
        raw[:, 0:width] = dot(tok[s], win[:, cols]).astype(BF16).astype(F32)
        for j in range(width // 128):
            lo = col0 + j * 128
            taps = convk_ref[:, lo : lo + 128] * 0.5
            bias = convb_ref[lo : lo + 128].reshape(1, 128) * 0.5

            def conv_body(c, carry):
                t0 = pl.multiple_of(c * Q + RIM - 8, 8)
                v = raw[pl.ds(t0, Q + 8), j * 128 : (j + 1) * 128]
                acc = v * taps[3:4]
                for back in range(1, KT):
                    acc = acc + pltpu.roll(v, back, 0) * taps[3 - back : 4 - back]
                h = acc[8:] + bias
                out = h + h * jnp.tanh(h)
                xs[s, pl.ds(pl.multiple_of(c * Q, 16), Q), lo : lo + 128] = out.astype(BF16)
                return carry

            lax.fori_loop(0, chunks, conv_body, 0)

    for s in range(series_here):
        produce(DI, 2 * N, s)

    def bt_body(ci, carry):
        s = ci // chunks
        t0 = pl.multiple_of((ci % chunks) * Q, 16)
        bt[ci] = xs[s, pl.ds(t0, Q), DI : DI + N].astype(F32).T.astype(BF16)
        return carry

    lax.fori_loop(0, nc, bt_body, 0)

    def i_copy(g, k, slot):
        return pltpu.make_async_remote_copy(
            src_ref=isend.at[g, k],
            dst_ref=irecv.at[g, slot],
            send_sem=i_ssem.at[g, k],
            recv_sem=i_rsem.at[g, slot],
            device_id=(k, ser),
            device_id_type=MESH,
        )

    def s_copy(g, k, slot):
        return pltpu.make_async_remote_copy(
            src_ref=ssend.at[g, k],
            dst_ref=srecv.at[g, slot],
            send_sem=s_ssem.at[g, k],
            recv_sem=s_rsem.at[g, slot],
            device_id=(k, ser),
            device_id_type=MESH,
        )

    def group(g):
        col0 = g * GC
        for s in range(series_here):
            produce(col0, GC, s)
            scur[s] = jnp.zeros((N, GC), F32)

            def inc_body(c, carry):
                ci = s * chunks + c
                t0 = pl.multiple_of(c * Q, 16)
                fx = dot(fhl[ci], eh[:, col0 : col0 + GC])
                wx = (xs[s, pl.ds(t0, Q), col0 : col0 + GC].astype(F32) * fx).astype(BF16)
                inc = dot(bt[ci], wx)
                cur = scur[s]
                sl[s, c, :, col0 : col0 + GC] = cur
                scur[s] = cur * rowx[pl.ds(ci, 1), col0 : col0 + GC] + inc
                return carry

            lax.fori_loop(0, chunks, inc_body, 0)
        parts = [scur[s].reshape(N // 8, 8, GC) for s in range(series_here)]
        isend[g] = jnp.concatenate(parts, axis=1).astype(BF16)

        @pl.when(me < n_tm - 1)
        def _():
            def send_i(k, carry):
                @pl.when(k != me)
                def _():
                    i_copy(g, k, me).start()

                return carry

            lax.fori_loop(0, n_tm, send_i, 0)

        irecv[g, me] = isend[g, me]

    def server(g):
        col0 = g * GC
        if g == 0:

            def wait_d(k, carry):
                @pl.when(k != me)
                def _():
                    d_copy(k, k).wait_recv()

                return carry

            lax.fori_loop(0, n_tm, wait_d, 0)
        dall = jnp.exp2(drecv[...].reshape(n_tm * 8, 128)[:, 0:H])
        dxs[...] = dot(hilo(dall), eh[:, col0 : col0 + GC]).reshape(n_tm, 8, GC)

        def emit(k, s0, s1):
            ssend[g, k] = jnp.concatenate([s0, s1], axis=0).astype(BF16)

            @pl.when((k != me) & (k > 0))
            def _():
                s_copy(g, k, me).start()

            @pl.when(k == me)
            def _():
                srecv[g, me] = jnp.concatenate([s0, s1], axis=0).astype(BF16)

        def scan_body(k, carry):
            s0, s1 = carry
            emit(k, s0, s1)

            @pl.when(k != me)
            def _():
                i_copy(g, k, k).wait_recv()

            part = irecv[g, k].astype(F32)
            s0 = s0 * dxs[k, 0:1, :] + part[0:8]
            s1 = s1 * dxs[k, 1:2, :] + part[8:16]
            return s0, s1

        zero = jnp.zeros((8, GC), F32)
        s0, s1 = lax.fori_loop(0, n_tm - 1, scan_body, (zero, zero))
        emit(n_tm - 1, s0, s1)

    def gates(s):
        def gate_body(i, carry):
            c0 = pl.multiple_of(i * 256, 256)
            h = dot(tok[s, RIM:, :], wgate[:, pl.ds(c0, 256)]) * 0.5
            sg[pl.ds(s * steps, steps), pl.ds(c0, 256)] = h + h * jnp.tanh(h)
            return carry

        lax.fori_loop(0, DI // 256, gate_body, 0)

    lanes1 = lax.broadcasted_iota(jnp.int32, (1, 128), 1)
    left = jnp.where(lanes1 < 64, 1.0, 0.0).astype(BF16)
    right = jnp.where(lanes1 < 64, 0.0, 1.0).astype(BF16)

    def intra(lo, hi):
        def intra_body(ci, carry):
            s = ci // chunks
            c = ci % chunks
            t0 = pl.multiple_of(c * Q, 16)
            r0 = pl.multiple_of(ci * Q, 16)
            cc = xs[s, pl.ds(t0, Q), DI + N : DI + 2 * N]
            sc = jnp.where(tri_r >= tri_c, dot(cc, bt[ci]), 0.0)
            for p in range(lo, hi):
                ws = []
                for h in (2 * p, 2 * p + 1):
                    d = cumc[ci, :, h : h + 1] - crt[ci, h : h + 1, :]
                    ws.append((jnp.exp2(jnp.minimum(d, 100.0)) * sc).astype(BF16))
                xp = xs[s, pl.ds(t0, Q), p * 128 : (p + 1) * 128]
                rhs = jnp.concatenate([xp * left, xp * right], axis=0)
                y = dot(jnp.concatenate(ws, axis=1), rhs)
                y = y + xp.astype(F32) * rowx[16:17, p * 128 : (p + 1) * 128]
                yb[pl.ds(r0, Q), p * 128 : (p + 1) * 128] = y
            return carry

        lax.fori_loop(0, nc, intra_body, 0)

    group(0)
    group(1)
    server(0)
    group(2)
    server(1)
    group(3)
    server(2)
    loads[3].wait()
    gates(0)
    server(3)
    gates(1)
    intra(0, H // 2)
    loads[4].wait()

    @pl.when(me == 0)
    def _():
        srecv[...] = jnp.zeros_like(srecv)

    for g in range(GROUPS):

        @pl.when(me > 0)
        def _():
            def wait_s(k, carry):
                @pl.when(k != me)
                def _():
                    s_copy(g, k, k).wait_recv()

                return carry

            lax.fori_loop(0, n_tm, wait_s, 0)

        got = srecv[g].astype(F32)
        for s in range(series_here):
            sin[s, :, g * GC : (g + 1) * GC] = got[:, 8 * s : 8 * s + 8, :].reshape(N, GC)

    def final_body(ci, carry):
        s = ci // chunks
        c = ci % chunks
        t0 = pl.multiple_of(c * Q, 16)
        r0 = pl.multiple_of(ci * Q, 16)
        cc = xs[s, pl.ds(t0, Q), DI + N : DI + 2 * N]
        ssq = jnp.zeros((Q, 128), F32)
        for g in range(2 * GROUPS):
            w = GC // 2
            cols = slice(g * w, (g + 1) * w)
            st = sin[s, :, cols] * rowx[pl.ds(8 + ci, 1), cols] + sl[s, c, :, cols]
            inter = dot(cc, st.astype(BF16))
            gx = dot(ghl[ci], eh[:, cols])
            y = yb[pl.ds(r0, Q), cols] + gx * inter
            gated = y * sg[pl.ds(r0, Q), cols]
            yb[pl.ds(r0, Q), cols] = gated
            sq = gated * gated
            for j in range(w // 128):
                ssq = ssq + sq[:, j * 128 : (j + 1) * 128]
        scale = lax.rsqrt(jnp.sum(ssq, axis=1, keepdims=True) * (1.0 / DI) + EPS)
        for j in range(DI // 256):
            cols = slice(j * 256, (j + 1) * 256)
            gain = gain_ref[cols].reshape(1, 256)
            nb[:, cols] = (yb[pl.ds(r0, Q), cols] * scale * gain).astype(BF16)
        live = jnp.where(lenv[s] > (me * steps + c * Q).astype(F32), 1.0, 0.0)[0:1, 0:1]
        res = dot(nb[...], wout[...]) * live
        o0 = pl.multiple_of(RIM + c * Q, 16)
        tok[s, pl.ds(o0, Q), :] = res.astype(BF16)
        pltpu.make_async_copy(
            tok.at[s, pl.ds(o0, Q), :], out_hbm.at[s, pl.ds(t0, Q), :], out_sem.at[ci]
        ).start()
        return carry

    lax.fori_loop(0, nc, final_body, 0)

    def drain_out(ci, carry):
        s = ci // chunks
        c = ci % chunks
        pltpu.make_async_copy(
            tok.at[s, pl.ds(pl.multiple_of(RIM + c * Q, 16), Q), :],
            out_hbm.at[s, pl.ds(pl.multiple_of(c * Q, 16), Q), :],
            out_sem.at[ci],
        ).wait()
        return carry

    lax.fori_loop(0, nc, drain_out, 0)

    def drain_len(k, carry):
        @pl.when(k != ser)
        def _():
            len_copy(k, ser).wait_send()

        return carry

    lax.fori_loop(0, n_ser, drain_len, 0)

    @pl.when(me < n_tm - 1)
    def _():
        for s in range(series_here):
            rim_copy(s).wait_send()

    def drain_tm(k, carry):
        @pl.when(k != me)
        def _():
            d_copy(k, me).wait_send()

        @pl.when((k != me) & (me < n_tm - 1))
        def _():
            for g in range(GROUPS):
                i_copy(g, k, me).wait_send()

        @pl.when((k != me) & (k > 0))
        def _():
            for g in range(GROUPS):
                s_copy(g, k, me).wait_send()

        return carry

    lax.fori_loop(0, n_tm, drain_tm, 0)


def body(
    n_tm,
    n_ser,
    tokens,
    gate_proj,
    input_proj,
    step_proj,
    conv_kernel,
    conv_bias,
    step_bias,
    decay_rate,
    skip_gain,
    norm_gain,
    out_proj,
    lengths,
    slot_series,
):
    series_here, steps, _ = tokens.shape
    chunks = steps // Q
    nc = series_here * chunks
    any_spec = pl.BlockSpec(memory_space=pl.ANY)
    vmem = pl.BlockSpec(memory_space=pltpu.VMEM)
    smem = pl.BlockSpec(memory_space=pltpu.SMEM)
    dma = pltpu.SemaphoreType.DMA
    scratch = [
        pltpu.VMEM((series_here, RIM + steps, D), BF16),
        pltpu.VMEM((D, W_IN), BF16),
        pltpu.VMEM((D, DI), BF16),
        pltpu.VMEM((DI, D), BF16),
        pltpu.VMEM((series_here, steps, W_IN), BF16),
        pltpu.VMEM((nc, N, Q), BF16),
        pltpu.VMEM((RIM + steps, GC), F32),
        pltpu.VMEM((nc, Q, H), F32),
        pltpu.VMEM((nc, H, Q), F32),
        pltpu.VMEM((nc, Q, 2 * H), BF16),
        pltpu.VMEM((nc, Q, 2 * H), BF16),
        pltpu.VMEM((2 * H, DI), BF16),
        pltpu.VMEM((32, H), F32),
        pltpu.VMEM((32, DI), F32),
        pltpu.VMEM((series_here, chunks, N, DI), F32),
        pltpu.VMEM((series_here, N, GC), F32),
        pltpu.VMEM((series_here, N, DI), F32),
        pltpu.VMEM((series_here * steps, DI), F32),
        pltpu.VMEM((series_here * steps, DI), F32),
        pltpu.VMEM((Q, DI), BF16),
        pltpu.VMEM((GROUPS, n_tm, 16, GC), BF16),
        pltpu.VMEM((GROUPS, n_tm, 16, GC), BF16),
        pltpu.VMEM((GROUPS, n_tm, 16, GC), BF16),
        pltpu.VMEM((GROUPS, n_tm, 16, GC), BF16),
        pltpu.VMEM((8, 128), F32),
        pltpu.VMEM((n_tm, 8, 128), F32),
        pltpu.VMEM((n_tm, 8, GC), F32),
        pltpu.VMEM((8, 128), jnp.int32),
        pltpu.VMEM((n_ser, 8, 128), jnp.int32),
        pltpu.VMEM((series_here, 8, 128), F32),
        dma((5,)),
        dma((nc,)),
        dma((n_ser,)),
        dma((n_ser,)),
        dma((series_here,)),
        dma((series_here,)),
        dma((n_tm,)),
        dma((n_tm,)),
        dma((GROUPS, n_tm)),
        dma((GROUPS, n_tm)),
        dma((GROUPS, n_tm)),
        dma((GROUPS, n_tm)),
    ]
    return pl.pallas_call(
        functools.partial(kernel, n_tm, n_ser, series_here, steps),
        out_shape=jax.ShapeDtypeStruct(tokens.shape, BF16),
        in_specs=[any_spec] * 3 + [vmem] * 7 + [any_spec] + [smem] * 2,
        out_specs=any_spec,
        scratch_shapes=scratch,
        compiler_params=pltpu.CompilerParams(
            collective_id=0,
            has_side_effects=True,
            vmem_limit_bytes=67_000_000,
        ),
        name="mixer",
    )(
        tokens,
        gate_proj,
        input_proj,
        step_proj,
        conv_kernel,
        conv_bias,
        step_bias,
        decay_rate,
        skip_gain,
        norm_gain,
        out_proj,
        lengths,
        slot_series,
    )


def solution(mesh):
    n_tm, n_ser = mesh.shape["tm"], mesh.shape["series"]
    in_specs = (P("series", "tm", None),) + (P(),) * 10 + (P("series"), P("series"))
    return jax.shard_map(
        functools.partial(body, n_tm, n_ser),
        mesh=mesh,
        in_specs=in_specs,
        out_specs=P("series", "tm", None),
        check_vma=False,
    )
```

```python
import functools
import math

import jax
import jax.numpy as jnp
from jax import lax
from jax.experimental import pallas as pl
from jax.experimental.pallas import tpu as pltpu
from jax.sharding import PartitionSpec as P

MESH = pl.DeviceIdType.MESH
F32 = jnp.float32
BF16 = jnp.bfloat16

D = 1024
DI = 2048
H = 32
N = 128
KT = 4
W_IN = DI + 2 * N
Q = 128
EPS = 1e-05
LOG2E = 1.4426950408889634
RIM = 16
GROUPS = 4
GC = DI // GROUPS
GATE_PIECES = 4
VMEM = 64_000_000


def dot(a, b, **kw):
    return jnp.dot(a, b, preferred_element_type=F32, **kw)


def scoped(name, f, *a):
    with jax.named_scope(name):
        return f(*a)


def expand(cols, first):
    lanes = lax.broadcasted_iota(jnp.int32, cols.shape, 1)
    index = jnp.where(lanes < 64, first, first + 1)
    return jnp.take_along_axis(cols, index, axis=1, mode="promise_in_bounds")


def kernel(
    n_tm,
    n_ser,
    series_here,
    steps,
    tokens_hbm,
    gate_hbm,
    in_hbm,
    stepw_ref,
    convk_ref,
    convb_ref,
    stepb_ref,
    rate_ref,
    skip_ref,
    gain_ref,
    out_w_hbm,
    len_smem,
    slot_smem,
    out_hbm,
    tok,
    win,
    wgate,
    wout,
    xs,
    bt,
    raw_a,
    raw_b,
    cumc,
    crt,
    scs,
    dts,
    rows,
    rowx,
    sl,
    ends,
    sin,
    ssq,
    ghl,
    eh,
    yb,
    sg,
    nb0,
    nb1,
    isend,
    irecv,
    ssend,
    srecv,
    dsend,
    drecv,
    dxs,
    lsend,
    lrecv,
    lenv,
    load_sem,
    out_sem,
    len_ssem,
    len_rsem,
    rim_ssem,
    rim_rsem,
    d_ssem,
    d_rsem,
    i_ssem,
    i_rsem,
    s_ssem,
    s_rsem,
):
    me = lax.axis_index("tm")
    ser = lax.axis_index("series")
    chunks = steps // Q
    nc = series_here * chunks
    nbs = (nb0, nb1)

    side = math.isqrt(n_tm)

    def away(d):
        x = lax.rem(me // side + d // side, side)
        return x * side + lax.rem(me + d, side)

    loads = []
    for s in range(series_here):
        loads.append(
            pltpu.make_async_copy(
                tokens_hbm.at[s], tok.at[s, pl.ds(RIM, steps), :], load_sem.at[s]
            )
        )
    loads.append(pltpu.make_async_copy(in_hbm, win, load_sem.at[2]))
    loads.append(pltpu.make_async_copy(out_w_hbm, wout, load_sem.at[3]))
    gate_loads = []
    for j in range(GATE_PIECES):
        gcols = pl.ds(j * (DI // GATE_PIECES), DI // GATE_PIECES)
        gate_loads.append(
            pltpu.make_async_copy(gate_hbm.at[:, gcols], wgate.at[:, gcols], load_sem.at[4 + j])
        )
    for c in [loads[0]] + gate_loads + loads[1:]:
        c.start()

    barrier = pltpu.get_barrier_semaphore()

    def greet_tm(k, carry):
        @pl.when(k != me)
        def _():
            pl.semaphore_signal(barrier, inc=1, device_id=(k, ser), device_id_type=MESH)

        return carry

    def greet_ser(k, carry):
        @pl.when(k != ser)
        def _():
            pl.semaphore_signal(barrier, inc=1, device_id=(me, k), device_id_type=MESH)

        return carry

    lax.fori_loop(0, n_tm, greet_tm, 0)
    lax.fori_loop(0, n_ser, greet_ser, 0)

    lane = lax.broadcasted_iota(jnp.int32, (8, 128), 1)
    lsend[...] = jnp.where(lane == 0, len_smem[0], jnp.where(lane == 1, len_smem[1], 0))
    er = lax.broadcasted_iota(jnp.int32, (2 * H, DI), 0)
    ec = lax.broadcasted_iota(jnp.int32, (2 * H, DI), 1)
    eh[...] = jnp.where((er % H) == ec // (DI // H), 1.0, 0.0).astype(BF16)
    dsend[...] = jnp.zeros_like(dsend)
    rows[...] = jnp.zeros_like(rows)

    def gates(s, lo, hi):
        for i in range(lo, hi):
            cols = slice(i * 256, (i + 1) * 256)
            if s == 0 and i % (DI // 256 // GATE_PIECES) == 0:
                gate_loads[i // (DI // 256 // GATE_PIECES)].wait()
            h = dot(tok[s, RIM:, :], wgate[:, cols]) * 0.5
            sg[s * steps : (s + 1) * steps, cols] = h + h * jnp.tanh(h)

    with jax.named_scope("barrier"):
        pl.semaphore_wait(barrier, n_tm + n_ser - 2)

    def len_copy(k, slot):
        return pltpu.make_async_remote_copy(
            src_ref=lsend,
            dst_ref=lrecv.at[slot],
            send_sem=len_ssem.at[0],
            recv_sem=len_rsem.at[0],
            device_id=(me, k),
            device_id_type=MESH,
        )

    def len_all():
        return pltpu.make_async_remote_copy(
            src_ref=lrecv.at[pl.ds(0, n_ser - 1)],
            dst_ref=lrecv.at[pl.ds(0, n_ser - 1)],
            send_sem=len_ssem.at[0],
            recv_sem=len_rsem.at[0],
            device_id=(me, ser),
            device_id_type=MESH,
        )

    def send_len(k, carry):
        @pl.when(k != ser)
        def _():
            len_copy(k, ser).start()

        return carry

    lax.fori_loop(0, n_ser, send_len, 0)
    lrecv[ser] = lsend[...]

    def rim_copy(s):
        return pltpu.make_async_remote_copy(
            src_ref=tokens_hbm.at[s, pl.ds(steps - RIM, RIM), :],
            dst_ref=tok.at[s, pl.ds(0, RIM), :],
            send_sem=rim_ssem.at[s],
            recv_sem=rim_rsem.at[s],
            device_id=(lax.rem(me + 1, n_tm), ser),
            device_id_type=MESH,
        )

    @pl.when(me < n_tm - 1)
    def _():
        for s in range(series_here):
            rim_copy(s).start()

    @pl.when(me == 0)
    def _():
        for s in range(series_here):
            tok[s, 0:RIM, :] = jnp.zeros((RIM, D), BF16)

    loads[0].wait()
    scoped("gates0", gates, 0, 0, 4)
    loads[1].wait()
    with jax.named_scope("lenwait"):
        len_all().wait_recv()
    for s in range(series_here):
        sid = slot_smem[s]
        found = jnp.zeros((8, 128), jnp.int32)
        for p in range(n_ser):
            hit = (lane < series_here) & (lane + series_here * p == sid)
            found = found + jnp.where(hit, lrecv[p], 0)
        lenv[s] = jnp.broadcast_to(
            jnp.sum(found.astype(F32), axis=1, keepdims=True), (8, 128)
        )

    tri_r = lax.broadcasted_iota(jnp.int32, (Q, Q), 0)
    tri_c = lax.broadcasted_iota(jnp.int32, (Q, Q), 1)

    def decays():
        eye = tri_r[0:H, 0:H] == tri_c[0:H, 0:H]

        def column(ref):
            wide = jnp.broadcast_to(ref[...].reshape(1, H), (H, H))
            return jnp.sum(jnp.where(eye, wide, 0.0), axis=1, keepdims=True)

        bias = column(stepb_ref)
        neg_rate = column(rate_ref) * (-LOG2E)
        for s in range(series_here):
            pre = lax.dot_general(
                stepw_ref[...],
                tok[s, RIM:, :],
                (((1,), (1,)), ((), ())),
                preferred_element_type=F32,
            )
            pre = pre + bias
            dt = jnp.maximum(pre, 0.0) + jnp.log1p(jnp.exp(-jnp.abs(pre)))
            for c in range(chunks):
                first = (me * steps + c * Q).astype(F32)
                live = jnp.where(lenv[s] > first, 1.0, 0.0)[0:1, :]
                ci = s * chunks + c
                dts[ci * H : (ci + 1) * H, :] = dt[:, c * Q : (c + 1) * Q] * live
        dt = dts[...]
        scaled = (dt.reshape(nc, H, Q) * neg_rate).reshape(nc * H, Q)
        upper = jnp.where(tri_r <= tri_c, 1.0, 0.0)
        cum = dot(scaled, upper, precision=lax.Precision.HIGHEST)
        lg = jnp.where(dt > 0.0, jnp.log(jnp.where(dt > 0.0, dt, 1.0)) * LOG2E, -1e30)
        crp = cum - lg
        crt[...] = crp.reshape(nc, H, Q)
        f = jnp.exp2(cum[:, Q - 1 : Q] - crp)
        g = jnp.exp2(cum)
        zero = jnp.zeros((128 - 3 * H, Q), F32)
        for ci in range(nc):
            r = slice(ci * H, (ci + 1) * H)
            col = jnp.concatenate([cum[r], f[r], g[r], zero], axis=0).T
            cumc[ci] = col
            high = col[:, 2 * H : 3 * H].astype(BF16)
            low = (col[:, 2 * H : 3 * H] - high.astype(F32)).astype(BF16)
            ghl[ci, :, 0:H] = high
            ghl[ci, :, H : 2 * H] = low

    scoped("decays", decays)

    r8 = lax.broadcasted_iota(jnp.int32, (8, H), 0)
    ecl = jnp.zeros((8, H), F32)
    ebef = jnp.zeros((8, H), F32)
    dtot = jnp.zeros((8, H), F32)
    for s in range(series_here):
        before = jnp.zeros((1, H), F32)
        for c in range(chunks):
            ci = s * chunks + c
            last = cumc[ci, Q - 1 : Q, 0:H]
            ecl = jnp.where(r8 == ci, jnp.exp2(last), ecl)
            ebef = jnp.where(r8 == ci, jnp.exp2(before), ebef)
            before = before + last
        dtot = jnp.where(r8 == s, before, dtot)
    dsend[:, 0:H] = dtot
    rows[0:8, 0:H] = ecl
    rows[8:16, 0:H] = ebef
    rows[16:24, 0:H] = jnp.broadcast_to(skip_ref[...].reshape(1, H), (8, H))
    for p in range(H // 2):
        rowx[:, p * 128 : (p + 1) * 128] = expand(rows[...], 2 * p)

    def to_peers(src, dst, ssem, rsem):
        def send(d, carry):
            k = away(d)
            pltpu.make_async_remote_copy(
                src_ref=src(k),
                dst_ref=dst.at[me],
                send_sem=ssem,
                recv_sem=rsem,
                device_id=(k, ser),
                device_id_type=MESH,
            ).start()
            return carry

        lax.fori_loop(1, n_tm, send, 0)

    def all_peers(dst, ssem, rsem):
        others = dst.at[pl.ds(0, n_tm - 1)]
        return pltpu.make_async_remote_copy(
            src_ref=others,
            dst_ref=others,
            send_sem=ssem,
            recv_sem=rsem,
            device_id=(me, ser),
            device_id_type=MESH,
        )

    d_all = all_peers(drecv, d_ssem.at[0], d_rsem.at[0])
    i_all = [all_peers(irecv.at[g], i_ssem.at[g], i_rsem.at[g]) for g in range(GROUPS)]
    s_all = [all_peers(srecv.at[g], s_ssem.at[g], s_rsem.at[g]) for g in range(GROUPS)]
    to_peers(lambda k: dsend, drecv, d_ssem.at[0], d_rsem.at[0])
    drecv[me] = dsend[...]

    @pl.when(me > 0)
    def _():
        for s in range(series_here):
            rim_copy(s).wait_recv()

    loads[2].wait()

    def project(raw, s, col0, at):
        raw[s, :, at : at + 256] = (
            dot(tok[s], win[:, col0 + at : col0 + at + 256]).astype(BF16).astype(F32)
        )

    def convolve(raw, s, col0, at):
        lo = col0 + at
        taps = convk_ref[:, lo : lo + 128] * 0.5
        bias = convb_ref[lo : lo + 128].reshape(1, 128) * 0.5
        for c in range(chunks):
            t0 = c * Q
            v = raw[s, t0 + RIM - 8 : t0 + RIM + Q, at : at + 128]
            acc = v * taps[3:4]
            for back in range(1, KT):
                acc = acc + pltpu.roll(v, back, 0) * taps[3 - back : 4 - back]
            h = acc[8:] + bias
            xs[s, t0 : t0 + Q, lo : lo + 128] = (h + h * jnp.tanh(h)).astype(BF16)

    def lead():
        for s in range(series_here):
            project(raw_b, s, DI, 0)
        for s in range(series_here):
            for half in range(2):
                project(raw_a, s, 0, half * 256)
                convolve(raw_b, s, DI, half * 128)
            for c in range(chunks):
                ci = s * chunks + c
                b = xs[s, c * Q : (c + 1) * Q, DI : DI + N]
                bt[ci] = b.astype(F32).T.astype(BF16)
                cc = xs[s, c * Q : (c + 1) * Q, DI + N : DI + 2 * N]
                scs[ci] = jnp.where(tri_r >= tri_c, dot(cc, bt[ci]), 0.0)

    scoped("lead", lead)

    def group(g):
        col0 = g * GC
        here, ahead = (raw_a, raw_b) if g % 2 == 0 else (raw_b, raw_a)
        for s in range(series_here):
            for half in range(2):
                at = half * 256
                if g + 1 < GROUPS:
                    project(ahead, s, col0 + GC, at)
                else:
                    gates(0, 4 + 2 * s + half, 5 + 2 * s + half)
                for j in range(2):
                    convolve(here, s, col0, at + j * 128)
                hcols = slice(col0 + at, col0 + at + 256)
                for c in range(chunks):
                    ci = s * chunks + c
                    head = (col0 + at) // 64
                    fx = jnp.concatenate(
                        [expand(cumc[ci], H + head + 2 * j) for j in range(2)], axis=1
                    )
                    x = xs[s, c * Q : (c + 1) * Q, hcols].astype(F32)
                    inc = dot(bt[ci], (x * fx).astype(BF16))
                    if c > 0:
                        inc = inc + sl[s, c - 1, :, hcols] * rowx[ci : ci + 1, hcols]
                    if c + 1 < chunks:
                        sl[s, c, :, hcols] = inc
                    else:
                        ends[s, :, at : at + 256] = inc
        parts = [ends[s].reshape(N // 8, 8, GC) for s in range(series_here)]
        isend[g] = jnp.concatenate(parts, axis=1).astype(BF16)

        to_peers(lambda k: isend.at[g, k], irecv.at[g], i_ssem.at[g], i_rsem.at[g])
        irecv[g, me] = isend[g, me]

    def server(g):
        col0 = g * GC
        if g == 0:
            d_all.wait_recv()
        dall = jnp.exp2(drecv[...].reshape(n_tm * 8, 128))
        for j in range(GC // 128):
            wide = expand(dall, (col0 + j * 128) // 64)
            dxs[:, :, j * 128 : (j + 1) * 128] = wide.reshape(n_tm, 8, 128)

        i_all[g].wait_recv()
        s0 = s1 = jnp.zeros((8, GC), F32)
        for k in range(n_tm):
            ssend[g, k] = jnp.concatenate([s0, s1], axis=0).astype(BF16)
            if k + 1 < n_tm:
                part = irecv[g, k].astype(F32)
                s0 = s0 * dxs[k, 0:1, :] + part[0:8]
                s1 = s1 * dxs[k, 1:2, :] + part[8:16]
        srecv[g, me] = ssend[g, me]
        to_peers(lambda k: ssend.at[g, k], srecv.at[g], s_ssem.at[g], s_rsem.at[g])

    lanes1 = lax.broadcasted_iota(jnp.int32, (1, 128), 1)
    left = jnp.where(lanes1 < 64, 1.0, 0.0).astype(BF16)
    right = jnp.where(lanes1 < 64, 0.0, 1.0).astype(BF16)

    def intra(lo, hi):
        def intra_chunk(ci):
            s = ci // chunks
            t0 = pl.multiple_of((ci % chunks) * Q, 16)
            r0 = pl.multiple_of(ci * Q, 16)
            for p in range(H // 2):
                ws = []
                for h in (2 * p, 2 * p + 1):
                    d = cumc[ci, :, h : h + 1] - crt[ci, h : h + 1, :]
                    ws.append((jnp.exp2(jnp.minimum(d, 100.0)) * scs[ci]).astype(BF16))
                xp = xs[s, pl.ds(t0, Q), p * 128 : (p + 1) * 128]
                rhs = jnp.concatenate([xp * left, xp * right], axis=0)
                y = dot(jnp.concatenate(ws, axis=1), rhs)
                y = y + xp.astype(F32) * rowx[16:17, p * 128 : (p + 1) * 128]
                yb[pl.ds(r0, Q), p * 128 : (p + 1) * 128] = y

        def intra_body(i, carry):
            for half in range(2):
                g0 = pl.multiple_of((2 * i + half) * 256, 256)
                h = dot(tok[1, RIM:, :], wgate[:, pl.ds(g0, 256)]) * 0.5
                sg[steps : 2 * steps, pl.ds(g0, 256)] = h + h * jnp.tanh(h)
                intra_chunk(2 * i + half)
            return carry

        lax.fori_loop(lo, hi, intra_body, 0)

    scoped("group0", group, 0)
    scoped("group1", group, 1)
    scoped("group2", group, 2)
    scoped("server0", server, 0)
    scoped("group3", group, 3)
    scoped("server1", server, 1)
    scoped("intra0", intra, 0, nc // 4)
    scoped("server2", server, 2)
    scoped("intra1", intra, nc // 4, nc // 2)
    scoped("server3", server, 3)
    loads[3].wait()

    def arrive(g):
        s_all[g].wait_recv()
        got = srecv[g].astype(F32)
        for s in range(series_here):
            sin[s] = got[:, 8 * s : 8 * s + 8, :].reshape(N, GC)

    def mix(g, s, c):
        ci = s * chunks + c
        r = slice(ci * Q, (ci + 1) * Q)
        cc = xs[s, c * Q : (c + 1) * Q, DI + N : DI + 2 * N]
        total = None if g == 0 else ssq[r, :]
        for half in range(2):
            at = half * 256
            cols = slice(g * GC + at, g * GC + at + 256)
            st = sin[s, :, at : at + 256]
            if c > 0:
                st = st * rowx[8 + ci : 9 + ci, cols] + sl[s, c - 1, :, cols]
            inter = dot(cc, st.astype(BF16))
            gx = dot(ghl[ci], eh[:, cols])
            gated = (yb[r, cols] + gx * inter) * sg[r, cols]
            gain = gain_ref[cols].reshape(1, 256)
            nbs[s][c * Q : (c + 1) * Q, at : at + 256] = (gated * gain).astype(BF16)
            sq = gated * gated
            for j in range(2):
                piece = sq[:, j * 128 : (j + 1) * 128]
                total = piece if total is None else total + piece
        ssq[r, :] = total

    def row_scale(s):
        rs = slice(s * steps, (s + 1) * steps)
        mean = jnp.sum(ssq[rs, :], axis=1, keepdims=True) * (1.0 / DI)
        scale = lax.rsqrt(mean + EPS)
        for c in range(chunks):
            live = jnp.where(lenv[s] > (me * steps + c * Q).astype(F32), 1.0, 0.0)[0:1, 0:1]
            piece = scale[c * Q : (c + 1) * Q] * live
            ssq[s * steps + c * Q : s * steps + (c + 1) * Q, :] = jnp.broadcast_to(piece, (Q, 128))

    def leave(g, s, n):
        acc = raw_a if n < 2 else raw_b
        at = (n % 2) * 256
        part = dot(nbs[s][...], wout[g * GC : (g + 1) * GC, n * 256 : (n + 1) * 256])
        if g > 0:
            part = part + acc[s, 0:steps, at : at + 256]
        if g < GROUPS - 1:
            acc[s, 0:steps, at : at + 256] = part
            return
        for j in range(2):
            res = part[:, j * 128 : (j + 1) * 128] * ssq[s * steps : (s + 1) * steps, :]
            lo = n * 256 + j * 128
            tok[s, RIM : RIM + steps, lo : lo + 128] = res.astype(BF16)

    def out_copy(s):
        return pltpu.make_async_copy(
            tok.at[s, pl.ds(RIM, steps), :], out_hbm.at[s], out_sem.at[s]
        )

    for g in range(GROUPS):
        scoped("arrive", arrive, g)
        with jax.named_scope("final"):
            for c in range(chunks):
                mix(g, 0, c)
                if g > 0:
                    leave(g - 1, 1, c)
            if g == GROUPS - 1:
                row_scale(0)
            for c in range(chunks):
                mix(g, 1, c)
                leave(g, 0, c)
    out_copy(0).start()
    with jax.named_scope("last"):
        row_scale(1)
        for c in range(chunks):
            leave(GROUPS - 1, 1, c)
    out_copy(1).start()

    with jax.named_scope("drain"):
        for s in range(series_here):
            out_copy(s).wait()

    len_all().wait_send()

    @pl.when(me < n_tm - 1)
    def _():
        for s in range(series_here):
            rim_copy(s).wait_send()

    d_all.wait_send()
    for g in range(GROUPS):
        i_all[g].wait_send()
        s_all[g].wait_send()


def body(
    n_tm,
    n_ser,
    tokens,
    gate_proj,
    input_proj,
    step_proj,
    conv_kernel,
    conv_bias,
    step_bias,
    decay_rate,
    skip_gain,
    norm_gain,
    out_proj,
    lengths,
    slot_series,
):
    series_here, steps, _ = tokens.shape
    chunks = steps // Q
    nc = series_here * chunks
    any_spec = pl.BlockSpec(memory_space=pl.ANY)
    vmem = pl.BlockSpec(memory_space=pltpu.VMEM)
    smem = pl.BlockSpec(memory_space=pltpu.SMEM)
    dma = pltpu.SemaphoreType.DMA
    scratch = [
        pltpu.VMEM((series_here, RIM + steps, D), BF16),
        pltpu.VMEM((D, W_IN), BF16),
        pltpu.VMEM((D, DI), BF16),
        pltpu.VMEM((DI, D), BF16),
        pltpu.VMEM((series_here, steps, W_IN), BF16),
        pltpu.VMEM((nc, N, Q), BF16),
        pltpu.VMEM((series_here, RIM + steps, GC), F32),
        pltpu.VMEM((series_here, RIM + steps, GC), F32),
        pltpu.VMEM((nc, Q, 128), F32),
        pltpu.VMEM((nc, H, Q), F32),
        pltpu.VMEM((nc, Q, Q), F32),
        pltpu.VMEM((nc * H, Q), F32),
        pltpu.VMEM((24, 128), F32),
        pltpu.VMEM((24, DI), F32),
        pltpu.VMEM((series_here, chunks - 1, N, DI), F32),
        pltpu.VMEM((series_here, N, GC), F32),
        pltpu.VMEM((series_here, N, GC), F32),
        pltpu.VMEM((series_here * steps, 128), F32),
        pltpu.VMEM((nc, Q, 2 * H), BF16),
        pltpu.VMEM((2 * H, DI), BF16),
        pltpu.VMEM((series_here * steps, DI), F32),
        pltpu.VMEM((series_here * steps, DI), F32),
        pltpu.VMEM((steps, GC), BF16),
        pltpu.VMEM((steps, GC), BF16),
        pltpu.VMEM((GROUPS, n_tm, 16, GC), BF16),
        pltpu.VMEM((GROUPS, n_tm, 16, GC), BF16),
        pltpu.VMEM((GROUPS, n_tm, 16, GC), BF16),
        pltpu.VMEM((GROUPS, n_tm, 16, GC), BF16),
        pltpu.VMEM((8, 128), F32),
        pltpu.VMEM((n_tm, 8, 128), F32),
        pltpu.VMEM((n_tm, 8, GC), F32),
        pltpu.VMEM((8, 128), jnp.int32),
        pltpu.VMEM((n_ser, 8, 128), jnp.int32),
        pltpu.VMEM((series_here, 8, 128), F32),
        dma((4 + GATE_PIECES,)),
        dma((nc,)),
        dma((1,)),
        dma((1,)),
        dma((series_here,)),
        dma((series_here,)),
        dma((1,)),
        dma((1,)),
        dma((GROUPS,)),
        dma((GROUPS,)),
        dma((GROUPS,)),
        dma((GROUPS,)),
    ]
    return pl.pallas_call(
        functools.partial(kernel, n_tm, n_ser, series_here, steps),
        out_shape=jax.ShapeDtypeStruct(tokens.shape, BF16),
        in_specs=[any_spec] * 3 + [vmem] * 7 + [any_spec] + [smem] * 2,
        out_specs=any_spec,
        scratch_shapes=scratch,
        compiler_params=pltpu.CompilerParams(
            collective_id=0,
            has_side_effects=True,
            vmem_limit_bytes=VMEM,
        ),
        name="mixer",
    )(
        tokens,
        gate_proj,
        input_proj,
        step_proj.T,
        conv_kernel,
        conv_bias,
        step_bias,
        decay_rate,
        skip_gain,
        norm_gain,
        out_proj,
        lengths,
        slot_series,
    )


def solution(mesh):
    n_tm, n_ser = mesh.shape["tm"], mesh.shape["series"]
    in_specs = (P("series", "tm", None),) + (P(),) * 10 + (P("series"), P("series"))
    return jax.shard_map(
        functools.partial(body, n_tm, n_ser),
        mesh=mesh,
        in_specs=in_specs,
        out_specs=P("series", "tm", None),
        check_vma=False,
    )
```

```python
import functools
import math

import jax
import jax.numpy as jnp
from jax import lax
from jax.experimental import pallas as pl
from jax.experimental.pallas import tpu as pltpu
from jax.sharding import PartitionSpec as P

MESH = pl.DeviceIdType.MESH
F32 = jnp.float32
BF16 = jnp.bfloat16

D = 1024
DI = 2048
H = 32
N = 128
KT = 4
W_IN = DI + 2 * N
Q = 128
EPS = 1e-05
LOG2E = 1.4426950408889634
RIM = 16
GROUPS = 4
GC = DI // GROUPS
GATE_PIECES = 4
VMEM = 64_000_000


def dot(a, b, **kw):
    return jnp.dot(a, b, preferred_element_type=F32, **kw)


def scoped(name, f, *a):
    with jax.named_scope(name):
        return f(*a)


def expand(cols, first):
    lanes = lax.broadcasted_iota(jnp.int32, cols.shape, 1)
    index = jnp.where(lanes < 64, first, first + 1)
    return jnp.take_along_axis(cols, index, axis=1, mode="promise_in_bounds")


def kernel(
    n_tm,
    n_ser,
    series_here,
    steps,
    tokens_hbm,
    gate_hbm,
    in_hbm,
    stepw_ref,
    convk_ref,
    convb_ref,
    stepb_ref,
    rate_ref,
    skip_ref,
    gain_ref,
    out_w_hbm,
    len_smem,
    slot_smem,
    out_ref,
    tok,
    win,
    wgate,
    wout,
    xs,
    bt,
    raw_a,
    raw_b,
    cumc,
    crt,
    scs,
    dts,
    rows,
    rowx,
    sl,
    ends,
    sin,
    ssq,
    ghl,
    eh,
    yb,
    sg,
    nb0,
    nb1,
    isend,
    irecv,
    ssend,
    srecv,
    dsend,
    drecv,
    dxs,
    lsend,
    lrecv,
    lenv,
    load_sem,
    len_ssem,
    len_rsem,
    rim_ssem,
    rim_rsem,
    d_ssem,
    d_rsem,
    i_ssem,
    i_rsem,
    s_ssem,
    s_rsem,
):
    me = lax.axis_index("tm")
    ser = lax.axis_index("series")
    chunks = steps // Q
    nc = series_here * chunks
    nbs = (nb0, nb1)

    side = math.isqrt(n_tm)

    def away(d):
        x = lax.rem(me // side + d // side, side)
        return x * side + lax.rem(me + d, side)

    loads = []
    for s in range(series_here):
        loads.append(
            pltpu.make_async_copy(
                tokens_hbm.at[s], tok.at[s, pl.ds(RIM, steps), :], load_sem.at[s]
            )
        )
    loads.append(pltpu.make_async_copy(in_hbm, win, load_sem.at[2]))
    loads.append(pltpu.make_async_copy(out_w_hbm, wout, load_sem.at[3]))
    gate_loads = []
    for j in range(GATE_PIECES):
        gcols = pl.ds(j * (DI // GATE_PIECES), DI // GATE_PIECES)
        gate_loads.append(
            pltpu.make_async_copy(gate_hbm.at[:, gcols], wgate.at[:, gcols], load_sem.at[4 + j])
        )
    for c in [loads[0]] + gate_loads + loads[1:]:
        c.start()

    barrier = pltpu.get_barrier_semaphore()

    def greet_tm(k, carry):
        @pl.when(k != me)
        def _():
            pl.semaphore_signal(barrier, inc=1, device_id=(k, ser), device_id_type=MESH)

        return carry

    def greet_ser(k, carry):
        @pl.when(k != ser)
        def _():
            pl.semaphore_signal(barrier, inc=1, device_id=(me, k), device_id_type=MESH)

        return carry

    lax.fori_loop(0, n_tm, greet_tm, 0)
    lax.fori_loop(0, n_ser, greet_ser, 0)

    lane = lax.broadcasted_iota(jnp.int32, (8, 128), 1)
    lsend[...] = jnp.where(lane == 0, len_smem[0], jnp.where(lane == 1, len_smem[1], 0))
    er = lax.broadcasted_iota(jnp.int32, (2 * H, DI), 0)
    ec = lax.broadcasted_iota(jnp.int32, (2 * H, DI), 1)
    eh[...] = jnp.where((er % H) == ec // (DI // H), 1.0, 0.0).astype(BF16)
    dsend[...] = jnp.zeros_like(dsend)
    rows[...] = jnp.zeros_like(rows)

    def gates(s, lo, hi):
        for i in range(lo, hi):
            cols = slice(i * 256, (i + 1) * 256)
            if s == 0 and i % (DI // 256 // GATE_PIECES) == 0:
                gate_loads[i // (DI // 256 // GATE_PIECES)].wait()
            h = dot(tok[s, RIM:, :], wgate[:, cols]) * 0.5
            sg[s * steps : (s + 1) * steps, cols] = h + h * jnp.tanh(h)

    with jax.named_scope("barrier"):
        pl.semaphore_wait(barrier, n_tm + n_ser - 2)

    def len_copy(k, slot):
        return pltpu.make_async_remote_copy(
            src_ref=lsend,
            dst_ref=lrecv.at[slot],
            send_sem=len_ssem.at[0],
            recv_sem=len_rsem.at[0],
            device_id=(me, k),
            device_id_type=MESH,
        )

    def len_all():
        return pltpu.make_async_remote_copy(
            src_ref=lrecv.at[pl.ds(0, n_ser - 1)],
            dst_ref=lrecv.at[pl.ds(0, n_ser - 1)],
            send_sem=len_ssem.at[0],
            recv_sem=len_rsem.at[0],
            device_id=(me, ser),
            device_id_type=MESH,
        )

    def send_len(k, carry):
        @pl.when(k != ser)
        def _():
            len_copy(k, ser).start()

        return carry

    lax.fori_loop(0, n_ser, send_len, 0)
    lrecv[ser] = lsend[...]

    def rim_copy(s):
        return pltpu.make_async_remote_copy(
            src_ref=tokens_hbm.at[s, pl.ds(steps - RIM, RIM), :],
            dst_ref=tok.at[s, pl.ds(0, RIM), :],
            send_sem=rim_ssem.at[s],
            recv_sem=rim_rsem.at[s],
            device_id=(lax.rem(me + 1, n_tm), ser),
            device_id_type=MESH,
        )

    @pl.when(me < n_tm - 1)
    def _():
        for s in range(series_here):
            rim_copy(s).start()

    @pl.when(me == 0)
    def _():
        for s in range(series_here):
            tok[s, 0:RIM, :] = jnp.zeros((RIM, D), BF16)

    tri_r = lax.broadcasted_iota(jnp.int32, (Q, Q), 0)
    tri_c = lax.broadcasted_iota(jnp.int32, (Q, Q), 1)

    def column(ref):
        wide = jnp.broadcast_to(ref[...].reshape(1, H), (H, H))
        eye = tri_r[0:H, 0:H] == tri_c[0:H, 0:H]
        return jnp.sum(jnp.where(eye, wide, 0.0), axis=1, keepdims=True)

    def softplus():
        bias = column(stepb_ref)
        for s in range(series_here):
            pre = lax.dot_general(
                stepw_ref[...],
                tok[s, RIM:, :],
                (((1,), (1,)), ((), ())),
                preferred_element_type=F32,
            )
            pre = pre + bias
            dt = jnp.maximum(pre, 0.0) + jnp.log1p(jnp.exp(-jnp.abs(pre)))
            for c in range(chunks):
                ci = s * chunks + c
                dts[ci * H : (ci + 1) * H, :] = dt[:, c * Q : (c + 1) * Q]

    loads[0].wait()
    scoped("gates0", gates, 0, 0, 4)
    loads[1].wait()
    scoped("softplus", softplus)
    with jax.named_scope("lenwait"):
        len_all().wait_recv()
    for s in range(series_here):
        sid = slot_smem[s]
        found = jnp.zeros((8, 128), jnp.int32)
        for p in range(n_ser):
            hit = (lane < series_here) & (lane + series_here * p == sid)
            found = found + jnp.where(hit, lrecv[p], 0)
        lenv[s] = jnp.broadcast_to(
            jnp.sum(found.astype(F32), axis=1, keepdims=True), (8, 128)
        )

    def decays():
        for s in range(series_here):
            for c in range(chunks):
                first = (me * steps + c * Q).astype(F32)
                live = jnp.where(lenv[s] > first, 1.0, 0.0)[0:1, :]
                r = slice((s * chunks + c) * H, (s * chunks + c + 1) * H)
                dts[r, :] = dts[r, :] * live
        neg_rate = column(rate_ref) * (-LOG2E)
        dt = dts[...]
        scaled = (dt.reshape(nc, H, Q) * neg_rate).reshape(nc * H, Q)
        upper = jnp.where(tri_r <= tri_c, 1.0, 0.0)
        cum = dot(scaled, upper, precision=lax.Precision.HIGHEST)
        lg = jnp.where(dt > 0.0, jnp.log(jnp.where(dt > 0.0, dt, 1.0)) * LOG2E, -1e30)
        crp = cum - lg
        crt[...] = crp.reshape(nc, H, Q)
        f = jnp.exp2(cum[:, Q - 1 : Q] - crp)
        g = jnp.exp2(cum)
        zero = jnp.zeros((128 - 3 * H, Q), F32)
        for ci in range(nc):
            r = slice(ci * H, (ci + 1) * H)
            col = jnp.concatenate([cum[r], f[r], g[r], zero], axis=0).T
            cumc[ci] = col
            high = col[:, 2 * H : 3 * H].astype(BF16)
            low = (col[:, 2 * H : 3 * H] - high.astype(F32)).astype(BF16)
            ghl[ci, :, 0:H] = high
            ghl[ci, :, H : 2 * H] = low

    scoped("decays", decays)

    r8 = lax.broadcasted_iota(jnp.int32, (8, H), 0)
    ecl = jnp.zeros((8, H), F32)
    ebef = jnp.zeros((8, H), F32)
    dtot = jnp.zeros((8, H), F32)
    for s in range(series_here):
        before = jnp.zeros((1, H), F32)
        for c in range(chunks):
            ci = s * chunks + c
            last = cumc[ci, Q - 1 : Q, 0:H]
            ecl = jnp.where(r8 == ci, jnp.exp2(last), ecl)
            ebef = jnp.where(r8 == ci, jnp.exp2(before), ebef)
            before = before + last
        dtot = jnp.where(r8 == s, before, dtot)
    dsend[:, 0:H] = dtot
    rows[0:8, 0:H] = ecl
    rows[8:16, 0:H] = ebef
    rows[16:24, 0:H] = jnp.broadcast_to(skip_ref[...].reshape(1, H), (8, H))
    for p in range(H // 2):
        rowx[:, p * 128 : (p + 1) * 128] = expand(rows[...], 2 * p)

    def to_peers(src, dst, ssem, rsem):
        def send(d, carry):
            k = away(d)
            pltpu.make_async_remote_copy(
                src_ref=src(k),
                dst_ref=dst.at[me],
                send_sem=ssem,
                recv_sem=rsem,
                device_id=(k, ser),
                device_id_type=MESH,
            ).start()
            return carry

        lax.fori_loop(1, n_tm, send, 0)

    def all_peers(dst, ssem, rsem):
        others = dst.at[pl.ds(0, n_tm - 1)]
        return pltpu.make_async_remote_copy(
            src_ref=others,
            dst_ref=others,
            send_sem=ssem,
            recv_sem=rsem,
            device_id=(me, ser),
            device_id_type=MESH,
        )

    d_all = all_peers(drecv, d_ssem.at[0], d_rsem.at[0])
    i_all = [all_peers(irecv.at[g], i_ssem.at[g], i_rsem.at[g]) for g in range(GROUPS)]
    s_all = [all_peers(srecv.at[g], s_ssem.at[g], s_rsem.at[g]) for g in range(GROUPS)]
    to_peers(lambda k: dsend, drecv, d_ssem.at[0], d_rsem.at[0])
    drecv[me] = dsend[...]

    @pl.when(me > 0)
    def _():
        for s in range(series_here):
            rim_copy(s).wait_recv()

    loads[2].wait()

    def project(raw, s, col0, at):
        raw[s, :, at : at + 256] = (
            dot(tok[s], win[:, col0 + at : col0 + at + 256]).astype(BF16).astype(F32)
        )

    def convolve(raw, s, col0, at):
        lo = col0 + at
        taps = convk_ref[:, lo : lo + 128] * 0.5
        bias = convb_ref[lo : lo + 128].reshape(1, 128) * 0.5
        for c in range(chunks):
            t0 = c * Q
            v = raw[s, t0 + RIM - 8 : t0 + RIM + Q, at : at + 128]
            acc = v * taps[3:4]
            for back in range(1, KT):
                acc = acc + pltpu.roll(v, back, 0) * taps[3 - back : 4 - back]
            h = acc[8:] + bias
            xs[s, t0 : t0 + Q, lo : lo + 128] = (h + h * jnp.tanh(h)).astype(BF16)

    def lead():
        for s in range(series_here):
            project(raw_b, s, DI, 0)
        for s in range(series_here):
            for half in range(2):
                project(raw_a, s, 0, half * 256)
                convolve(raw_b, s, DI, half * 128)
            for c in range(chunks):
                ci = s * chunks + c
                b = xs[s, c * Q : (c + 1) * Q, DI : DI + N]
                bt[ci] = b.astype(F32).T.astype(BF16)
                cc = xs[s, c * Q : (c + 1) * Q, DI + N : DI + 2 * N]
                scs[ci] = jnp.where(tri_r >= tri_c, dot(cc, bt[ci]), 0.0)

    scoped("lead", lead)

    def group(g):
        col0 = g * GC
        here, ahead = (raw_a, raw_b) if g % 2 == 0 else (raw_b, raw_a)
        for s in range(series_here):
            for half in range(2):
                at = half * 256
                if g + 1 < GROUPS:
                    project(ahead, s, col0 + GC, at)
                else:
                    gates(0, 4 + 2 * s + half, 5 + 2 * s + half)
                for j in range(2):
                    convolve(here, s, col0, at + j * 128)
                hcols = slice(col0 + at, col0 + at + 256)
                for c in range(chunks):
                    ci = s * chunks + c
                    head = (col0 + at) // 64
                    fx = jnp.concatenate(
                        [expand(cumc[ci], H + head + 2 * j) for j in range(2)], axis=1
                    )
                    x = xs[s, c * Q : (c + 1) * Q, hcols].astype(F32)
                    inc = dot(bt[ci], (x * fx).astype(BF16))
                    if c > 0:
                        inc = inc + sl[s, c - 1, :, hcols] * rowx[ci : ci + 1, hcols]
                    if c + 1 < chunks:
                        sl[s, c, :, hcols] = inc
                    else:
                        ends[s, :, at : at + 256] = inc
        parts = [ends[s].reshape(N // 8, 8, GC) for s in range(series_here)]
        isend[g] = jnp.concatenate(parts, axis=1).astype(BF16)

        to_peers(lambda k: isend.at[g, k], irecv.at[g], i_ssem.at[g], i_rsem.at[g])
        irecv[g, me] = isend[g, me]

    def server(g):
        col0 = g * GC
        if g == 0:
            d_all.wait_recv()
        dall = jnp.exp2(drecv[...].reshape(n_tm * 8, 128))
        for j in range(GC // 128):
            wide = expand(dall, (col0 + j * 128) // 64)
            dxs[:, :, j * 128 : (j + 1) * 128] = wide.reshape(n_tm, 8, 128)

        i_all[g].wait_recv()
        s0 = s1 = jnp.zeros((8, GC), F32)
        for k in range(n_tm):
            ssend[g, k] = jnp.concatenate([s0, s1], axis=0).astype(BF16)
            if k + 1 < n_tm:
                part = irecv[g, k].astype(F32)
                s0 = s0 * dxs[k, 0:1, :] + part[0:8]
                s1 = s1 * dxs[k, 1:2, :] + part[8:16]
        srecv[g, me] = ssend[g, me]
        to_peers(lambda k: ssend.at[g, k], srecv.at[g], s_ssem.at[g], s_rsem.at[g])

    lanes1 = lax.broadcasted_iota(jnp.int32, (1, 128), 1)
    left = jnp.where(lanes1 < 64, 1.0, 0.0).astype(BF16)
    right = jnp.where(lanes1 < 64, 0.0, 1.0).astype(BF16)

    def intra(lo, hi):
        def intra_chunk(ci):
            s = ci // chunks
            t0 = pl.multiple_of((ci % chunks) * Q, 16)
            r0 = pl.multiple_of(ci * Q, 16)
            for p in range(H // 2):
                ws = []
                for h in (2 * p, 2 * p + 1):
                    d = cumc[ci, :, h : h + 1] - crt[ci, h : h + 1, :]
                    ws.append((jnp.exp2(jnp.minimum(d, 100.0)) * scs[ci]).astype(BF16))
                xp = xs[s, pl.ds(t0, Q), p * 128 : (p + 1) * 128]
                rhs = jnp.concatenate([xp * left, xp * right], axis=0)
                y = dot(jnp.concatenate(ws, axis=1), rhs)
                y = y + xp.astype(F32) * rowx[16:17, p * 128 : (p + 1) * 128]
                yb[pl.ds(r0, Q), p * 128 : (p + 1) * 128] = y

        def intra_body(i, carry):
            for half in range(2):
                g0 = pl.multiple_of((2 * i + half) * 256, 256)
                h = dot(tok[1, RIM:, :], wgate[:, pl.ds(g0, 256)]) * 0.5
                sg[steps : 2 * steps, pl.ds(g0, 256)] = h + h * jnp.tanh(h)
                intra_chunk(2 * i + half)
            return carry

        lax.fori_loop(lo, hi, intra_body, 0)

    scoped("group0", group, 0)
    scoped("group1", group, 1)
    scoped("group2", group, 2)
    scoped("server0", server, 0)
    scoped("group3", group, 3)
    scoped("server1", server, 1)
    scoped("intra0", intra, 0, nc // 4)
    scoped("server2", server, 2)
    scoped("intra1", intra, nc // 4, nc // 2)
    scoped("server3", server, 3)
    loads[3].wait()

    def arrive(g):
        s_all[g].wait_recv()
        got = srecv[g].astype(F32)
        for s in range(series_here):
            sin[s] = got[:, 8 * s : 8 * s + 8, :].reshape(N, GC)

    def mix(g, s, c):
        ci = s * chunks + c
        r = slice(ci * Q, (ci + 1) * Q)
        cc = xs[s, c * Q : (c + 1) * Q, DI + N : DI + 2 * N]
        total = None if g == 0 else ssq[r, :]
        for half in range(2):
            at = half * 256
            cols = slice(g * GC + at, g * GC + at + 256)
            st = sin[s, :, at : at + 256]
            if c > 0:
                st = st * rowx[8 + ci : 9 + ci, cols] + sl[s, c - 1, :, cols]
            inter = dot(cc, st.astype(BF16))
            gx = dot(ghl[ci], eh[:, cols])
            gated = (yb[r, cols] + gx * inter) * sg[r, cols]
            gain = gain_ref[cols].reshape(1, 256)
            nbs[s][c * Q : (c + 1) * Q, at : at + 256] = (gated * gain).astype(BF16)
            sq = gated * gated
            for j in range(2):
                piece = sq[:, j * 128 : (j + 1) * 128]
                total = piece if total is None else total + piece
        ssq[r, :] = total

    def row_scale(s):
        rs = slice(s * steps, (s + 1) * steps)
        mean = jnp.sum(ssq[rs, :], axis=1, keepdims=True) * (1.0 / DI)
        scale = lax.rsqrt(mean + EPS)
        for c in range(chunks):
            live = jnp.where(lenv[s] > (me * steps + c * Q).astype(F32), 1.0, 0.0)[0:1, 0:1]
            piece = scale[c * Q : (c + 1) * Q] * live
            ssq[s * steps + c * Q : s * steps + (c + 1) * Q, :] = jnp.broadcast_to(piece, (Q, 128))

    def leave(g, s, n):
        acc = raw_a if n < 2 else raw_b
        at = (n % 2) * 256
        part = dot(nbs[s][...], wout[g * GC : (g + 1) * GC, n * 256 : (n + 1) * 256])
        if g > 0:
            part = part + acc[s, 0:steps, at : at + 256]
        if g < GROUPS - 1:
            acc[s, 0:steps, at : at + 256] = part
            return
        for j in range(2):
            res = part[:, j * 128 : (j + 1) * 128] * ssq[s * steps : (s + 1) * steps, :]
            lo = n * 256 + j * 128
            out_ref[s, :, lo : lo + 128] = res.astype(BF16)

    for g in range(GROUPS):
        scoped("arrive", arrive, g)
        with jax.named_scope("final"):
            for c in range(chunks):
                mix(g, 0, c)
                if g > 0:
                    leave(g - 1, 1, c)
            if g == GROUPS - 1:
                row_scale(0)
            for c in range(chunks):
                mix(g, 1, c)
                leave(g, 0, c)
    with jax.named_scope("last"):
        row_scale(1)
        for c in range(chunks):
            leave(GROUPS - 1, 1, c)

    len_all().wait_send()

    @pl.when(me < n_tm - 1)
    def _():
        for s in range(series_here):
            rim_copy(s).wait_send()

    d_all.wait_send()
    for g in range(GROUPS):
        i_all[g].wait_send()
        s_all[g].wait_send()


def body(
    n_tm,
    n_ser,
    tokens,
    gate_proj,
    input_proj,
    step_proj,
    conv_kernel,
    conv_bias,
    step_bias,
    decay_rate,
    skip_gain,
    norm_gain,
    out_proj,
    lengths,
    slot_series,
):
    series_here, steps, _ = tokens.shape
    chunks = steps // Q
    nc = series_here * chunks
    any_spec = pl.BlockSpec(memory_space=pl.ANY)
    vmem = pl.BlockSpec(memory_space=pltpu.VMEM)
    smem = pl.BlockSpec(memory_space=pltpu.SMEM)
    dma = pltpu.SemaphoreType.DMA
    scratch = [
        pltpu.VMEM((series_here, RIM + steps, D), BF16),
        pltpu.VMEM((D, W_IN), BF16),
        pltpu.VMEM((D, DI), BF16),
        pltpu.VMEM((DI, D), BF16),
        pltpu.VMEM((series_here, steps, W_IN), BF16),
        pltpu.VMEM((nc, N, Q), BF16),
        pltpu.VMEM((series_here, RIM + steps, GC), F32),
        pltpu.VMEM((series_here, RIM + steps, GC), F32),
        pltpu.VMEM((nc, Q, 128), F32),
        pltpu.VMEM((nc, H, Q), F32),
        pltpu.VMEM((nc, Q, Q), F32),
        pltpu.VMEM((nc * H, Q), F32),
        pltpu.VMEM((24, 128), F32),
        pltpu.VMEM((24, DI), F32),
        pltpu.VMEM((series_here, chunks - 1, N, DI), F32),
        pltpu.VMEM((series_here, N, GC), F32),
        pltpu.VMEM((series_here, N, GC), F32),
        pltpu.VMEM((series_here * steps, 128), F32),
        pltpu.VMEM((nc, Q, 2 * H), BF16),
        pltpu.VMEM((2 * H, DI), BF16),
        pltpu.VMEM((series_here * steps, DI), F32),
        pltpu.VMEM((series_here * steps, DI), F32),
        pltpu.VMEM((steps, GC), BF16),
        pltpu.VMEM((steps, GC), BF16),
        pltpu.VMEM((GROUPS, n_tm, 16, GC), BF16),
        pltpu.VMEM((GROUPS, n_tm, 16, GC), BF16),
        pltpu.VMEM((GROUPS, n_tm, 16, GC), BF16),
        pltpu.VMEM((GROUPS, n_tm, 16, GC), BF16),
        pltpu.VMEM((8, 128), F32),
        pltpu.VMEM((n_tm, 8, 128), F32),
        pltpu.VMEM((n_tm, 8, GC), F32),
        pltpu.VMEM((8, 128), jnp.int32),
        pltpu.VMEM((n_ser, 8, 128), jnp.int32),
        pltpu.VMEM((series_here, 8, 128), F32),
        dma((4 + GATE_PIECES,)),
        dma((1,)),
        dma((1,)),
        dma((series_here,)),
        dma((series_here,)),
        dma((1,)),
        dma((1,)),
        dma((GROUPS,)),
        dma((GROUPS,)),
        dma((GROUPS,)),
        dma((GROUPS,)),
    ]
    return pl.pallas_call(
        functools.partial(kernel, n_tm, n_ser, series_here, steps),
        out_shape=pltpu.VMEM(tokens.shape, BF16),
        in_specs=[any_spec] * 3 + [vmem] * 7 + [any_spec] + [smem] * 2,
        out_specs=vmem,
        scratch_shapes=scratch,
        compiler_params=pltpu.CompilerParams(
            collective_id=0,
            has_side_effects=True,
            vmem_limit_bytes=VMEM,
        ),
        name="mixer",
    )(
        tokens,
        gate_proj,
        input_proj,
        step_proj.T,
        conv_kernel,
        conv_bias,
        step_bias,
        decay_rate,
        skip_gain,
        norm_gain,
        out_proj,
        lengths,
        slot_series,
    )


def solution(mesh):
    n_tm, n_ser = mesh.shape["tm"], mesh.shape["series"]
    in_specs = (P("series", "tm", None),) + (P(),) * 10 + (P("series"), P("series"))
    return jax.shard_map(
        functools.partial(body, n_tm, n_ser),
        mesh=mesh,
        in_specs=in_specs,
        out_specs=P("series", "tm", None),
        check_vma=False,
    )
```

```python
import functools
import math

import jax
import jax.numpy as jnp
from jax import lax
from jax.experimental import pallas as pl
from jax.experimental.pallas import tpu as pltpu
from jax.sharding import PartitionSpec as P

MESH = pl.DeviceIdType.MESH
F32 = jnp.float32
BF16 = jnp.bfloat16

D = 1024
DI = 2048
H = 32
N = 128
KT = 4
W_IN = DI + 2 * N
Q = 128
EPS = 1e-05
LOG2E = 1.4426950408889634
RIM = 16
SENT = 8
GROUPS = 4
GC = DI // GROUPS
GATE_PIECES = 4
VMEM = 64_000_000


def dot(a, b, **kw):
    return jnp.dot(a, b, preferred_element_type=F32, **kw)


def scoped(name, f, *a):
    with jax.named_scope(name):
        return f(*a)


def expand(cols, first):
    lanes = lax.broadcasted_iota(jnp.int32, cols.shape, 1)
    index = jnp.where(lanes < 64, first, first + 1)
    return jnp.take_along_axis(cols, index, axis=1, mode="promise_in_bounds")


def kernel(
    n_tm,
    n_ser,
    series_here,
    steps,
    tokens_hbm,
    gate_hbm,
    in_hbm,
    stepw_ref,
    convk_ref,
    convb_ref,
    stepb_ref,
    rate_ref,
    skip_ref,
    gain_ref,
    out_w_hbm,
    len_smem,
    slot_smem,
    out_ref,
    tok,
    win,
    wgate,
    wout,
    xs,
    bt,
    raw_a,
    raw_b,
    cumc,
    crt,
    scs,
    dts,
    rows,
    rowx,
    sl,
    ends,
    sin,
    ssq,
    ghl,
    eh,
    yb,
    sg,
    nb0,
    nb1,
    isend,
    irecv,
    ssend,
    srecv,
    dsend,
    drecv,
    dxs,
    lsend,
    lrecv,
    lenv,
    load_sem,
    len_ssem,
    len_rsem,
    rim_ssem,
    rim_rsem,
    d_ssem,
    d_rsem,
    i_ssem,
    i_rsem,
    s_ssem,
    s_rsem,
):
    me = lax.axis_index("tm")
    ser = lax.axis_index("series")
    chunks = steps // Q
    nc = series_here * chunks
    nbs = (nb0, nb1)

    side = math.isqrt(n_tm)

    origin = me // n_tm

    def away(d):
        x = lax.rem(me // side + d // side, side)
        return x * side + lax.rem(me + d, side)

    loads = []
    for s in range(series_here):
        loads.append(
            pltpu.make_async_copy(
                tokens_hbm.at[s], tok.at[s, pl.ds(RIM, steps), :], load_sem.at[s]
            )
        )
    loads.append(pltpu.make_async_copy(in_hbm, win, load_sem.at[2]))
    loads.append(pltpu.make_async_copy(out_w_hbm, wout, load_sem.at[3]))
    gate_loads = []
    for j in range(GATE_PIECES):
        gcols = pl.ds(j * (DI // GATE_PIECES), DI // GATE_PIECES)
        gate_loads.append(
            pltpu.make_async_copy(gate_hbm.at[:, gcols], wgate.at[:, gcols], load_sem.at[4 + j])
        )
    for c in loads[:2] + gate_loads + loads[2:]:
        c.start()

    barrier = pltpu.get_barrier_semaphore()

    def greet_tm(k, carry):
        @pl.when(k != me)
        def _():
            pl.semaphore_signal(barrier, inc=1, device_id=(k, ser), device_id_type=MESH)

        return carry

    def greet_ser(k, carry):
        @pl.when(k != ser)
        def _():
            pl.semaphore_signal(barrier, inc=1, device_id=(me, k), device_id_type=MESH)

        return carry

    lax.fori_loop(0, n_tm, greet_tm, 0)
    lax.fori_loop(0, n_ser, greet_ser, 0)

    lane = lax.broadcasted_iota(jnp.int32, (8, 128), 1)
    lsend[...] = jnp.where(lane == 0, len_smem[0], jnp.where(lane == 1, len_smem[1], 0))
    er = lax.broadcasted_iota(jnp.int32, (2 * H, DI), 0)
    ec = lax.broadcasted_iota(jnp.int32, (2 * H, DI), 1)
    eh[...] = jnp.where((er % H) == ec // (DI // H), 1.0, 0.0).astype(BF16)
    dsend[...] = jnp.zeros_like(dsend)
    rows[...] = jnp.zeros_like(rows)

    def gates(s, lo, hi):
        for i in range(lo, hi):
            cols = slice(i * 256, (i + 1) * 256)
            if s == 0 and i % (DI // 256 // GATE_PIECES) == 0:
                gate_loads[i // (DI // 256 // GATE_PIECES)].wait()
            h = dot(tok[s, RIM:, :], wgate[:, cols]) * 0.5
            sg[s * steps : (s + 1) * steps, cols] = h + h * jnp.tanh(h)

    with jax.named_scope("barrier"):
        pl.semaphore_wait(barrier, n_tm + n_ser - 2)

    def len_copy(k, slot):
        return pltpu.make_async_remote_copy(
            src_ref=lsend,
            dst_ref=lrecv.at[slot],
            send_sem=len_ssem.at[0],
            recv_sem=len_rsem.at[0],
            device_id=(me, k),
            device_id_type=MESH,
        )

    def len_all():
        return pltpu.make_async_remote_copy(
            src_ref=lrecv.at[pl.ds(0, n_ser - 1)],
            dst_ref=lrecv.at[pl.ds(0, n_ser - 1)],
            send_sem=len_ssem.at[0],
            recv_sem=len_rsem.at[0],
            device_id=(me, ser),
            device_id_type=MESH,
        )

    def send_len(k, carry):
        @pl.when(k != ser)
        def _():
            len_copy(k, ser).start()

        return carry

    lax.fori_loop(0, n_ser, send_len, 0)
    lrecv[ser] = lsend[...]

    def rim_copy(s):
        return pltpu.make_async_remote_copy(
            src_ref=tok.at[s, pl.ds(RIM + steps - SENT, SENT), :],
            dst_ref=tok.at[s, pl.ds(RIM - SENT, SENT), :],
            send_sem=rim_ssem.at[s],
            recv_sem=rim_rsem.at[s],
            device_id=(lax.rem(me + 1, n_tm), ser),
            device_id_type=MESH,
        )

    for s in range(series_here):
        loads[s].wait()
        tok[s, 0 : RIM - SENT, :] = jnp.zeros((RIM - SENT, D), BF16)

    @pl.when(me < n_tm - 1)
    def _():
        for s in range(series_here):
            rim_copy(s).start()

    @pl.when(me == 0)
    def _():
        for s in range(series_here):
            tok[s, RIM - SENT : RIM, :] = jnp.zeros((SENT, D), BF16)

    tri_r = lax.broadcasted_iota(jnp.int32, (Q, Q), 0)
    tri_c = lax.broadcasted_iota(jnp.int32, (Q, Q), 1)

    def column(ref):
        wide = jnp.broadcast_to(ref[...].reshape(1, H), (H, H))
        eye = tri_r[0:H, 0:H] == tri_c[0:H, 0:H]
        return jnp.sum(jnp.where(eye, wide, 0.0), axis=1, keepdims=True)

    def softplus():
        bias = column(stepb_ref)
        for s in range(series_here):
            pre = lax.dot_general(
                stepw_ref[...],
                tok[s, RIM:, :],
                (((1,), (1,)), ((), ())),
                preferred_element_type=F32,
            )
            pre = pre + bias
            dt = jnp.maximum(pre, 0.0) + jnp.log1p(jnp.exp(-jnp.abs(pre)))
            for c in range(chunks):
                ci = s * chunks + c
                dts[ci * H : (ci + 1) * H, :] = dt[:, c * Q : (c + 1) * Q]

    scoped("gates0", gates, 0, 0, 4)
    scoped("softplus", softplus)
    def decays():
        for s in range(series_here):
            for c in range(chunks):
                first = (me * steps + c * Q).astype(F32)
                live = jnp.where(lenv[s] > first, 1.0, 0.0)[0:1, :]
                r = slice((s * chunks + c) * H, (s * chunks + c + 1) * H)
                dts[r, :] = dts[r, :] * live
        neg_rate = column(rate_ref) * (-LOG2E)
        dt = dts[...]
        scaled = (dt.reshape(nc, H, Q) * neg_rate).reshape(nc * H, Q)
        upper = jnp.where(tri_r <= tri_c, 1.0, 0.0)
        cum = dot(scaled, upper, precision=lax.Precision.HIGHEST)
        lg = jnp.where(dt > 0.0, jnp.log(jnp.where(dt > 0.0, dt, 1.0)) * LOG2E, -1e30)
        crp = cum - lg
        crt[...] = crp.reshape(nc, H, Q)
        f = jnp.exp2(cum[:, Q - 1 : Q] - crp)
        g = jnp.exp2(cum)
        zero = jnp.zeros((128 - 3 * H, Q), F32)
        for ci in range(nc):
            r = slice(ci * H, (ci + 1) * H)
            col = jnp.concatenate([cum[r], f[r], g[r], zero], axis=0).T
            cumc[ci] = col
            high = col[:, 2 * H : 3 * H].astype(BF16)
            low = (col[:, 2 * H : 3 * H] - high.astype(F32)).astype(BF16)
            ghl[ci, :, 0:H] = high
            ghl[ci, :, H : 2 * H] = low

    def row_values():
        r8 = lax.broadcasted_iota(jnp.int32, (8, H), 0)
        ecl = jnp.zeros((8, H), F32)
        ebef = jnp.zeros((8, H), F32)
        dtot = jnp.zeros((8, H), F32)
        for s in range(series_here):
            before = jnp.zeros((1, H), F32)
            for c in range(chunks):
                ci = s * chunks + c
                last = cumc[ci, Q - 1 : Q, 0:H]
                ecl = jnp.where(r8 == ci, jnp.exp2(last), ecl)
                ebef = jnp.where(r8 == ci, jnp.exp2(before), ebef)
                before = before + last
            dtot = jnp.where(r8 == s, before, dtot)
        dsend[:, 0:H] = dtot
        rows[0:8, 0:H] = ecl
        rows[8:16, 0:H] = ebef
        rows[16:24, 0:H] = jnp.broadcast_to(skip_ref[...].reshape(1, H), (8, H))
        for p in range(H // 2):
            rowx[:, p * 128 : (p + 1) * 128] = expand(rows[...], 2 * p)

    def to_peers(src, dst, ssem, rsem):
        def send(d, carry):
            k = away(d)
            pltpu.make_async_remote_copy(
                src_ref=src(k),
                dst_ref=dst.at[me],
                send_sem=ssem,
                recv_sem=rsem,
                device_id=(k, ser),
                device_id_type=MESH,
            ).start()
            return carry

        lax.fori_loop(1, n_tm, send, 0)

    def all_peers(dst, ssem, rsem):
        others = dst.at[pl.ds(0, n_tm - 1)]
        return pltpu.make_async_remote_copy(
            src_ref=others,
            dst_ref=others,
            send_sem=ssem,
            recv_sem=rsem,
            device_id=(me, ser),
            device_id_type=MESH,
        )

    d_all = all_peers(drecv, d_ssem.at[0], d_rsem.at[0])
    i_all = [all_peers(irecv.at[g], i_ssem.at[g], i_rsem.at[g]) for g in range(GROUPS)]
    s_all = [all_peers(srecv.at[g], s_ssem.at[g], s_rsem.at[g]) for g in range(GROUPS)]

    with jax.named_scope("rimwait"):

        @pl.when(me > 0)
        def _():
            for s in range(series_here):
                rim_copy(s).wait_recv()

    with jax.named_scope("winwait"):
        loads[2].wait()

    def project(raw, s, col0, at):
        got = dot(tok[s], win[:, col0 + at : col0 + at + 256]).astype(BF16).astype(F32)
        for j in range(2):
            raw[s, at // 128 + j] = got[:, j * 128 : (j + 1) * 128]

    def convolve(raw, s, col0, at):
        lo = col0 + at
        taps = convk_ref[:, lo : lo + 128] * 0.5
        bias = convb_ref[lo : lo + 128].reshape(1, 128) * 0.5
        for c in range(chunks):
            t0 = c * Q
            h = bias
            for k in range(KT):
                v = raw[s, at // 128, pl.ds(origin + (t0 + RIM - KT + 1 + k), Q), :]
                h = h + v * taps[k : k + 1]
            xs[s, t0 : t0 + Q, lo : lo + 128] = (h + h * jnp.tanh(h)).astype(BF16)

    def lead():
        for s in range(series_here):
            project(raw_b, s, DI, 0)
        for s in range(series_here):
            for half in range(2):
                project(raw_a, s, 0, half * 256)
                convolve(raw_b, s, DI, half * 128)
            for c in range(chunks):
                ci = s * chunks + c
                b = xs[s, c * Q : (c + 1) * Q, DI : DI + N]
                bt[ci] = b.astype(F32).T.astype(BF16)
                cc = xs[s, c * Q : (c + 1) * Q, DI + N : DI + 2 * N]
                scs[ci] = jnp.where(tri_r >= tri_c, dot(cc, bt[ci]), 0.0)

    scoped("lead", lead)
    with jax.named_scope("lenwait"):
        len_all().wait_recv()
    for s in range(series_here):
        sid = slot_smem[s]
        found = jnp.zeros((8, 128), jnp.int32)
        for p in range(n_ser):
            hit = (lane < series_here) & (lane + series_here * p == sid)
            found = found + jnp.where(hit, lrecv[p], 0)
        lenv[s] = jnp.broadcast_to(
            jnp.sum(found.astype(F32), axis=1, keepdims=True), (8, 128)
        )


    def group(g):
        col0 = g * GC
        here, ahead = (raw_a, raw_b) if g % 2 == 0 else (raw_b, raw_a)
        if g == 0:
            decays()
            row_values()
        for s in range(series_here):
            for half in range(2):
                at = half * 256
                if g + 1 < GROUPS:
                    project(ahead, s, col0 + GC, at)
                else:
                    gates(0, 4 + 2 * s + half, 5 + 2 * s + half)
                for j in range(2):
                    convolve(here, s, col0, at + j * 128)
                hcols = slice(col0 + at, col0 + at + 256)
                for c in range(chunks):
                    ci = s * chunks + c
                    head = (col0 + at) // 64
                    fx = jnp.concatenate(
                        [expand(cumc[ci], H + head + 2 * j) for j in range(2)], axis=1
                    )
                    x = xs[s, c * Q : (c + 1) * Q, hcols].astype(F32)
                    inc = dot(bt[ci], (x * fx).astype(BF16))
                    if c > 0:
                        inc = inc + sl[s, c - 1, :, hcols] * rowx[ci : ci + 1, hcols]
                    if c + 1 < chunks:
                        sl[s, c, :, hcols] = inc
                    else:
                        ends[s, :, at : at + 256] = inc
        parts = [ends[s].reshape(N // 8, 8, GC) for s in range(series_here)]
        isend[g] = jnp.concatenate(parts, axis=1).astype(BF16)

        if g == 0:
            to_peers(lambda k: dsend, drecv, d_ssem.at[0], d_rsem.at[0])
            drecv[me] = dsend[...]
        to_peers(lambda k: isend.at[g, k], irecv.at[g], i_ssem.at[g], i_rsem.at[g])
        irecv[g, me] = isend[g, me]

    def server(g):
        col0 = g * GC
        if g == 0:
            d_all.wait_recv()
        dall = jnp.exp2(drecv[...].reshape(n_tm * 8, 128))
        for j in range(GC // 128):
            wide = expand(dall, (col0 + j * 128) // 64)
            dxs[:, :, j * 128 : (j + 1) * 128] = wide.reshape(n_tm, 8, 128)

        i_all[g].wait_recv()
        s0 = s1 = jnp.zeros((8, GC), F32)
        for k in range(n_tm):
            ssend[g, k] = jnp.concatenate([s0, s1], axis=0).astype(BF16)
            if k + 1 < n_tm:
                part = irecv[g, k].astype(F32)
                s0 = s0 * dxs[k, 0:1, :] + part[0:8]
                s1 = s1 * dxs[k, 1:2, :] + part[8:16]
        srecv[g, me] = ssend[g, me]
        to_peers(lambda k: ssend.at[g, k], srecv.at[g], s_ssem.at[g], s_rsem.at[g])

    lanes1 = lax.broadcasted_iota(jnp.int32, (1, 128), 1)
    left = jnp.where(lanes1 < 64, 1.0, 0.0).astype(BF16)
    right = jnp.where(lanes1 < 64, 0.0, 1.0).astype(BF16)

    def intra(lo, hi):
        def intra_chunk(ci):
            s = ci // chunks
            t0 = pl.multiple_of((ci % chunks) * Q, 16)
            r0 = pl.multiple_of(ci * Q, 16)
            for p in range(H // 2):
                ws = []
                for h in (2 * p, 2 * p + 1):
                    d = cumc[ci, :, h : h + 1] - crt[ci, h : h + 1, :]
                    ws.append((jnp.exp2(jnp.minimum(d, 100.0)) * scs[ci]).astype(BF16))
                xp = xs[s, pl.ds(t0, Q), p * 128 : (p + 1) * 128]
                rhs = jnp.concatenate([xp * left, xp * right], axis=0)
                y = dot(jnp.concatenate(ws, axis=1), rhs)
                y = y + xp.astype(F32) * rowx[16:17, p * 128 : (p + 1) * 128]
                yb[pl.ds(r0, Q), p * 128 : (p + 1) * 128] = y

        def intra_body(i, carry):
            for half in range(2):
                g0 = pl.multiple_of((2 * i + half) * 256, 256)
                h = dot(tok[1, RIM:, :], wgate[:, pl.ds(g0, 256)]) * 0.5
                sg[steps : 2 * steps, pl.ds(g0, 256)] = h + h * jnp.tanh(h)
                intra_chunk(2 * i + half)
            return carry

        lax.fori_loop(lo, hi, intra_body, 0)

    scoped("group0", group, 0)
    scoped("group1", group, 1)
    scoped("group2", group, 2)
    scoped("server0", server, 0)
    scoped("group3", group, 3)
    scoped("server1", server, 1)
    scoped("intra0", intra, 0, nc // 4)
    scoped("server2", server, 2)
    scoped("intra1", intra, nc // 4, nc // 2)
    scoped("server3", server, 3)
    loads[3].wait()

    def arrive(g):
        s_all[g].wait_recv()
        got = srecv[g].astype(F32)
        for s in range(series_here):
            sin[s] = got[:, 8 * s : 8 * s + 8, :].reshape(N, GC)

    def mix(g, s, c):
        ci = s * chunks + c
        r = slice(ci * Q, (ci + 1) * Q)
        cc = xs[s, c * Q : (c + 1) * Q, DI + N : DI + 2 * N]
        total = None if g == 0 else ssq[r, :]
        for half in range(2):
            at = half * 256
            cols = slice(g * GC + at, g * GC + at + 256)
            st = sin[s, :, at : at + 256]
            if c > 0:
                st = st * rowx[8 + ci : 9 + ci, cols] + sl[s, c - 1, :, cols]
            inter = dot(cc, st.astype(BF16))
            gx = dot(ghl[ci], eh[:, cols])
            gated = (yb[r, cols] + gx * inter) * sg[r, cols]
            gain = gain_ref[cols].reshape(1, 256)
            nbs[s][c * Q : (c + 1) * Q, at : at + 256] = (gated * gain).astype(BF16)
            sq = gated * gated
            for j in range(2):
                piece = sq[:, j * 128 : (j + 1) * 128]
                total = piece if total is None else total + piece
        ssq[r, :] = total

    def row_scale(s):
        rs = slice(s * steps, (s + 1) * steps)
        mean = jnp.sum(ssq[rs, :], axis=1, keepdims=True) * (1.0 / DI)
        scale = lax.rsqrt(mean + EPS)
        for c in range(chunks):
            live = jnp.where(lenv[s] > (me * steps + c * Q).astype(F32), 1.0, 0.0)[0:1, 0:1]
            piece = scale[c * Q : (c + 1) * Q] * live
            ssq[s * steps + c * Q : s * steps + (c + 1) * Q, :] = jnp.broadcast_to(piece, (Q, 128))

    def leave(g, s, n):
        acc = raw_a if n < 2 else raw_b
        at = (n % 2) * 2
        part = dot(nbs[s][...], wout[g * GC : (g + 1) * GC, n * 256 : (n + 1) * 256])
        for j in range(2):
            piece = part[:, j * 128 : (j + 1) * 128]
            if g > 0:
                piece = piece + acc[s, at + j, 0:steps, :]
            if g < GROUPS - 1:
                acc[s, at + j, 0:steps, :] = piece
            else:
                lo = n * 256 + j * 128
                res = piece * ssq[s * steps : (s + 1) * steps, :]
                out_ref[s, :, lo : lo + 128] = res.astype(BF16)

    for g in range(GROUPS):
        if g == GROUPS - 1:
            for c in range(chunks):
                leave(g - 1, 1, c)
        scoped("arrive", arrive, g)
        with jax.named_scope("final"):
            for c in range(chunks):
                mix(g, 0, c)
                if 0 < g < GROUPS - 1:
                    leave(g - 1, 1, c)
            if g == GROUPS - 1:
                row_scale(0)
            for c in range(chunks):
                mix(g, 1, c)
                leave(g, 0, c)
    with jax.named_scope("last"):
        row_scale(1)
        for c in range(chunks):
            leave(GROUPS - 1, 1, c)

    len_all().wait_send()

    @pl.when(me < n_tm - 1)
    def _():
        for s in range(series_here):
            rim_copy(s).wait_send()

    d_all.wait_send()
    for g in range(GROUPS):
        i_all[g].wait_send()
        s_all[g].wait_send()


def body(
    n_tm,
    n_ser,
    tokens,
    gate_proj,
    input_proj,
    step_proj,
    conv_kernel,
    conv_bias,
    step_bias,
    decay_rate,
    skip_gain,
    norm_gain,
    out_proj,
    lengths,
    slot_series,
):
    series_here, steps, _ = tokens.shape
    chunks = steps // Q
    nc = series_here * chunks
    any_spec = pl.BlockSpec(memory_space=pl.ANY)
    vmem = pl.BlockSpec(memory_space=pltpu.VMEM)
    smem = pl.BlockSpec(memory_space=pltpu.SMEM)
    dma = pltpu.SemaphoreType.DMA
    scratch = [
        pltpu.VMEM((series_here, RIM + steps, D), BF16),
        pltpu.VMEM((D, W_IN), BF16),
        pltpu.VMEM((D, DI), BF16),
        pltpu.VMEM((DI, D), BF16),
        pltpu.VMEM((series_here, steps, W_IN), BF16),
        pltpu.VMEM((nc, N, Q), BF16),
        pltpu.VMEM((series_here, GC // 128, RIM + steps, 128), F32),
        pltpu.VMEM((series_here, GC // 128, RIM + steps, 128), F32),
        pltpu.VMEM((nc, Q, 128), F32),
        pltpu.VMEM((nc, H, Q), F32),
        pltpu.VMEM((nc, Q, Q), F32),
        pltpu.VMEM((nc * H, Q), F32),
        pltpu.VMEM((24, 128), F32),
        pltpu.VMEM((24, DI), F32),
        pltpu.VMEM((series_here, chunks - 1, N, DI), F32),
        pltpu.VMEM((series_here, N, GC), F32),
        pltpu.VMEM((series_here, N, GC), F32),
        pltpu.VMEM((series_here * steps, 128), F32),
        pltpu.VMEM((nc, Q, 2 * H), BF16),
        pltpu.VMEM((2 * H, DI), BF16),
        pltpu.VMEM((series_here * steps, DI), F32),
        pltpu.VMEM((series_here * steps, DI), F32),
        pltpu.VMEM((steps, GC), BF16),
        pltpu.VMEM((steps, GC), BF16),
        pltpu.VMEM((GROUPS, n_tm, 16, GC), BF16),
        pltpu.VMEM((GROUPS, n_tm, 16, GC), BF16),
        pltpu.VMEM((GROUPS, n_tm, 16, GC), BF16),
        pltpu.VMEM((GROUPS, n_tm, 16, GC), BF16),
        pltpu.VMEM((8, 128), F32),
        pltpu.VMEM((n_tm, 8, 128), F32),
        pltpu.VMEM((n_tm, 8, GC), F32),
        pltpu.VMEM((8, 128), jnp.int32),
        pltpu.VMEM((n_ser, 8, 128), jnp.int32),
        pltpu.VMEM((series_here, 8, 128), F32),
        dma((4 + GATE_PIECES,)),
        dma((1,)),
        dma((1,)),
        dma((series_here,)),
        dma((series_here,)),
        dma((1,)),
        dma((1,)),
        dma((GROUPS,)),
        dma((GROUPS,)),
        dma((GROUPS,)),
        dma((GROUPS,)),
    ]
    return pl.pallas_call(
        functools.partial(kernel, n_tm, n_ser, series_here, steps),
        out_shape=pltpu.VMEM(tokens.shape, BF16),
        in_specs=[any_spec] * 3 + [vmem] * 7 + [any_spec] + [smem] * 2,
        out_specs=vmem,
        scratch_shapes=scratch,
        compiler_params=pltpu.CompilerParams(
            collective_id=0,
            has_side_effects=True,
            vmem_limit_bytes=VMEM,
        ),
        name="mixer",
    )(
        tokens,
        gate_proj,
        input_proj,
        step_proj.T,
        conv_kernel,
        conv_bias,
        step_bias,
        decay_rate,
        skip_gain,
        norm_gain,
        out_proj,
        lengths,
        slot_series,
    )


def solution(mesh):
    n_tm, n_ser = mesh.shape["tm"], mesh.shape["series"]
    in_specs = (P("series", "tm", None),) + (P(),) * 10 + (P("series"), P("series"))
    return jax.shard_map(
        functools.partial(body, n_tm, n_ser),
        mesh=mesh,
        in_specs=in_specs,
        out_specs=P("series", "tm", None),
        check_vma=False,
    )
```

```python
import functools
import math

import jax
import jax.numpy as jnp
from jax import lax
from jax.experimental import pallas as pl
from jax.experimental.pallas import tpu as pltpu
from jax.sharding import PartitionSpec as P

MESH = pl.DeviceIdType.MESH
F32 = jnp.float32
BF16 = jnp.bfloat16

D = 1024
DI = 2048
H = 32
N = 128
KT = 4
W_IN = DI + 2 * N
Q = 128
EPS = 1e-05
LOG2E = 1.4426950408889634
RIM = 16
SENT = 8
GROUPS = 4
GC = DI // GROUPS
GATE_PIECES = 4
VMEM = 64_000_000


def dot(a, b, **kw):
    return jnp.dot(a, b, preferred_element_type=F32, **kw)


def scoped(name, f, *a):
    with jax.named_scope(name):
        return f(*a)


def expand(cols, first):
    lanes = lax.broadcasted_iota(jnp.int32, cols.shape, 1)
    index = jnp.where(lanes < 64, first, first + 1)
    return jnp.take_along_axis(cols, index, axis=1, mode="promise_in_bounds")


def kernel(
    n_tm,
    n_ser,
    series_here,
    steps,
    tokens_hbm,
    gate_hbm,
    in_hbm,
    stepw_ref,
    convk_ref,
    convb_ref,
    stepb_ref,
    rate_ref,
    skip_ref,
    gain_ref,
    out_w_hbm,
    len_smem,
    slot_smem,
    out_ref,
    tok,
    win,
    wgate,
    wout,
    xs,
    bt,
    raw_a,
    raw_b,
    cumc,
    crt,
    scs,
    dts,
    rows,
    rowx,
    sl,
    ends,
    sin,
    ssq,
    ghl,
    eh,
    yb,
    sg,
    nb0,
    nb1,
    isend,
    irecv,
    ssend,
    srecv,
    dsend,
    drecv,
    dxs,
    lsend,
    lrecv,
    lenv,
    load_sem,
    len_ssem,
    len_rsem,
    rim_ssem,
    rim_rsem,
    d_ssem,
    d_rsem,
    i_ssem,
    i_rsem,
    s_ssem,
    s_rsem,
):
    me = lax.axis_index("tm")
    ser = lax.axis_index("series")
    chunks = steps // Q
    nc = series_here * chunks
    nbs = (nb0, nb1)

    side = math.isqrt(n_tm)

    origin = me // n_tm

    def away(d):
        x = lax.rem(me // side + d // side, side)
        return x * side + lax.rem(me + d, side)

    loads = []
    for s in range(series_here):
        loads.append(
            pltpu.make_async_copy(
                tokens_hbm.at[s], tok.at[s, pl.ds(RIM, steps), :], load_sem.at[s]
            )
        )
    loads.append(pltpu.make_async_copy(in_hbm, win, load_sem.at[2]))
    loads.append(pltpu.make_async_copy(out_w_hbm, wout, load_sem.at[3]))
    gate_loads = []
    for j in range(GATE_PIECES):
        gcols = pl.ds(j * (DI // GATE_PIECES), DI // GATE_PIECES)
        gate_loads.append(
            pltpu.make_async_copy(gate_hbm.at[:, gcols], wgate.at[:, gcols], load_sem.at[4 + j])
        )
    for c in loads[:2] + gate_loads + loads[2:]:
        c.start()

    barrier = pltpu.get_barrier_semaphore()

    def greet_tm(k, carry):
        @pl.when(k != me)
        def _():
            pl.semaphore_signal(barrier, inc=1, device_id=(k, ser), device_id_type=MESH)

        return carry

    def greet_ser(k, carry):
        @pl.when(k != ser)
        def _():
            pl.semaphore_signal(barrier, inc=1, device_id=(me, k), device_id_type=MESH)

        return carry

    lax.fori_loop(0, n_tm, greet_tm, 0)
    lax.fori_loop(0, n_ser, greet_ser, 0)

    lane = lax.broadcasted_iota(jnp.int32, (8, 128), 1)
    lsend[...] = jnp.where(lane == 0, len_smem[0], jnp.where(lane == 1, len_smem[1], 0))
    er = lax.broadcasted_iota(jnp.int32, (2 * H, DI), 0)
    ec = lax.broadcasted_iota(jnp.int32, (2 * H, DI), 1)
    eh[...] = jnp.where((er % H) == ec // (DI // H), 1.0, 0.0).astype(BF16)
    dsend[...] = jnp.zeros_like(dsend)
    rows[...] = jnp.zeros_like(rows)

    def gates(s, lo, hi):
        for i in range(lo, hi):
            cols = slice(i * 256, (i + 1) * 256)
            if s == 0 and i % (DI // 256 // GATE_PIECES) == 0:
                gate_loads[i // (DI // 256 // GATE_PIECES)].wait()
            h = dot(tok[s, RIM:, :], wgate[:, cols]) * 0.5
            sg[s * steps : (s + 1) * steps, cols] = h + h * jnp.tanh(h)

    with jax.named_scope("barrier"):
        pl.semaphore_wait(barrier, n_tm + n_ser - 2)

    def len_copy(k, slot):
        return pltpu.make_async_remote_copy(
            src_ref=lsend,
            dst_ref=lrecv.at[slot],
            send_sem=len_ssem.at[0],
            recv_sem=len_rsem.at[0],
            device_id=(me, k),
            device_id_type=MESH,
        )

    def len_all():
        return pltpu.make_async_remote_copy(
            src_ref=lrecv.at[pl.ds(0, n_ser - 1)],
            dst_ref=lrecv.at[pl.ds(0, n_ser - 1)],
            send_sem=len_ssem.at[0],
            recv_sem=len_rsem.at[0],
            device_id=(me, ser),
            device_id_type=MESH,
        )

    def send_len(k, carry):
        @pl.when(k != ser)
        def _():
            len_copy(k, ser).start()

        return carry

    lax.fori_loop(0, n_ser, send_len, 0)
    lrecv[ser] = lsend[...]

    def rim_copy(s):
        return pltpu.make_async_remote_copy(
            src_ref=tok.at[s, pl.ds(RIM + steps - SENT, SENT), :],
            dst_ref=tok.at[s, pl.ds(RIM - SENT, SENT), :],
            send_sem=rim_ssem.at[s],
            recv_sem=rim_rsem.at[s],
            device_id=(lax.rem(me + 1, n_tm), ser),
            device_id_type=MESH,
        )

    for s in range(series_here):
        loads[s].wait()
        tok[s, 0 : RIM - SENT, :] = jnp.zeros((RIM - SENT, D), BF16)

    @pl.when(me < n_tm - 1)
    def _():
        for s in range(series_here):
            rim_copy(s).start()

    @pl.when(me == 0)
    def _():
        for s in range(series_here):
            tok[s, RIM - SENT : RIM, :] = jnp.zeros((SENT, D), BF16)

    tri_r = lax.broadcasted_iota(jnp.int32, (Q, Q), 0)
    tri_c = lax.broadcasted_iota(jnp.int32, (Q, Q), 1)

    def column(ref):
        wide = jnp.broadcast_to(ref[...].reshape(1, H), (H, H))
        eye = tri_r[0:H, 0:H] == tri_c[0:H, 0:H]
        return jnp.sum(jnp.where(eye, wide, 0.0), axis=1, keepdims=True)

    def softplus():
        bias = column(stepb_ref)
        for s in range(series_here):
            pre = lax.dot_general(
                stepw_ref[...],
                tok[s, RIM:, :],
                (((1,), (1,)), ((), ())),
                preferred_element_type=F32,
            )
            pre = pre + bias
            dt = jnp.maximum(pre, 0.0) + jnp.log1p(jnp.exp(-jnp.abs(pre)))
            for c in range(chunks):
                ci = s * chunks + c
                dts[ci * H : (ci + 1) * H, :] = dt[:, c * Q : (c + 1) * Q]

    scoped("gates0", gates, 0, 0, 4)
    scoped("softplus", softplus)
    def decays():
        for s in range(series_here):
            for c in range(chunks):
                first = (me * steps + c * Q).astype(F32)
                live = jnp.where(lenv[s] > first, 1.0, 0.0)[0:1, :]
                r = slice((s * chunks + c) * H, (s * chunks + c + 1) * H)
                dts[r, :] = dts[r, :] * live
        neg_rate = column(rate_ref) * (-LOG2E)
        dt = dts[...]
        scaled = (dt.reshape(nc, H, Q) * neg_rate).reshape(nc * H, Q)
        upper = jnp.where(tri_r <= tri_c, 1.0, 0.0)
        cum = dot(scaled, upper, precision=lax.Precision.HIGHEST)
        lg = jnp.where(dt > 0.0, jnp.log(jnp.where(dt > 0.0, dt, 1.0)) * LOG2E, -1e30)
        crp = cum - lg
        crt[...] = crp.reshape(nc, H, Q)
        f = jnp.exp2(cum[:, Q - 1 : Q] - crp)
        g = jnp.exp2(cum)
        zero = jnp.zeros((128 - 3 * H, Q), F32)
        for ci in range(nc):
            r = slice(ci * H, (ci + 1) * H)
            col = jnp.concatenate([cum[r], f[r], g[r], zero], axis=0).T
            cumc[ci] = col
            high = col[:, 2 * H : 3 * H].astype(BF16)
            low = (col[:, 2 * H : 3 * H] - high.astype(F32)).astype(BF16)
            ghl[ci, :, 0:H] = high
            ghl[ci, :, H : 2 * H] = low

    def row_values():
        r8 = lax.broadcasted_iota(jnp.int32, (8, H), 0)
        ecl = jnp.zeros((8, H), F32)
        ebef = jnp.zeros((8, H), F32)
        dtot = jnp.zeros((8, H), F32)
        for s in range(series_here):
            before = jnp.zeros((1, H), F32)
            for c in range(chunks):
                ci = s * chunks + c
                last = cumc[ci, Q - 1 : Q, 0:H]
                ecl = jnp.where(r8 == ci, jnp.exp2(last), ecl)
                ebef = jnp.where(r8 == ci, jnp.exp2(before), ebef)
                before = before + last
            dtot = jnp.where(r8 == s, before, dtot)
        dsend[:, 0:H] = dtot
        rows[0:8, 0:H] = ecl
        rows[8:16, 0:H] = ebef
        rows[16:24, 0:H] = jnp.broadcast_to(skip_ref[...].reshape(1, H), (8, H))
        for p in range(H // 2):
            rowx[:, p * 128 : (p + 1) * 128] = expand(rows[...], 2 * p)

    def to_peers(src, dst, ssem, rsem):
        def send(d, carry):
            k = away(lax.rem(7 * d, n_tm))
            pltpu.make_async_remote_copy(
                src_ref=src(k),
                dst_ref=dst.at[me],
                send_sem=ssem,
                recv_sem=rsem,
                device_id=(k, ser),
                device_id_type=MESH,
            ).start()
            return carry

        lax.fori_loop(1, n_tm, send, 0)

    def all_peers(dst, ssem, rsem):
        others = dst.at[pl.ds(0, n_tm - 1)]
        return pltpu.make_async_remote_copy(
            src_ref=others,
            dst_ref=others,
            send_sem=ssem,
            recv_sem=rsem,
            device_id=(me, ser),
            device_id_type=MESH,
        )

    d_all = all_peers(drecv, d_ssem.at[0], d_rsem.at[0])
    i_all = [all_peers(irecv.at[g], i_ssem.at[g], i_rsem.at[g]) for g in range(GROUPS)]
    s_all = [all_peers(srecv.at[g], s_ssem.at[g], s_rsem.at[g]) for g in range(GROUPS)]

    with jax.named_scope("rimwait"):

        @pl.when(me > 0)
        def _():
            for s in range(series_here):
                rim_copy(s).wait_recv()

    with jax.named_scope("winwait"):
        loads[2].wait()

    def project(raw, s, col0, at):
        got = dot(tok[s], win[:, col0 + at : col0 + at + 256]).astype(BF16).astype(F32)
        for j in range(2):
            raw[s, at // 128 + j] = got[:, j * 128 : (j + 1) * 128]

    def convolve(raw, s, col0, at):
        lo = col0 + at
        taps = convk_ref[:, lo : lo + 128] * 0.5
        bias = convb_ref[lo : lo + 128].reshape(1, 128) * 0.5
        for c in range(chunks):
            t0 = c * Q
            h = bias
            for k in range(KT):
                v = raw[s, at // 128, pl.ds(origin + (t0 + RIM - KT + 1 + k), Q), :]
                h = h + v * taps[k : k + 1]
            xs[s, t0 : t0 + Q, lo : lo + 128] = (h + h * jnp.tanh(h)).astype(BF16)

    def lead():
        for s in range(series_here):
            project(raw_b, s, DI, 0)
        for s in range(series_here):
            for half in range(2):
                project(raw_a, s, 0, half * 256)
                convolve(raw_b, s, DI, half * 128)
            for c in range(chunks):
                ci = s * chunks + c
                b = xs[s, c * Q : (c + 1) * Q, DI : DI + N]
                bt[ci] = b.astype(F32).T.astype(BF16)
                cc = xs[s, c * Q : (c + 1) * Q, DI + N : DI + 2 * N]
                scs[ci] = jnp.where(tri_r >= tri_c, dot(cc, bt[ci]), 0.0)

    scoped("lead", lead)
    with jax.named_scope("lenwait"):
        len_all().wait_recv()
    for s in range(series_here):
        sid = slot_smem[s]
        found = jnp.zeros((8, 128), jnp.int32)
        for p in range(n_ser):
            hit = (lane < series_here) & (lane + series_here * p == sid)
            found = found + jnp.where(hit, lrecv[p], 0)
        lenv[s] = jnp.broadcast_to(
            jnp.sum(found.astype(F32), axis=1, keepdims=True), (8, 128)
        )


    def group(g):
        col0 = g * GC
        here, ahead = (raw_a, raw_b) if g % 2 == 0 else (raw_b, raw_a)
        if g == 0:
            decays()
            row_values()
        for s in range(series_here):
            for half in range(2):
                at = half * 256
                if g + 1 < GROUPS:
                    project(ahead, s, col0 + GC, at)
                else:
                    gates(0, 4 + 2 * s + half, 5 + 2 * s + half)
                for j in range(2):
                    convolve(here, s, col0, at + j * 128)
                hcols = slice(col0 + at, col0 + at + 256)
                for c in range(chunks):
                    ci = s * chunks + c
                    head = (col0 + at) // 64
                    fx = jnp.concatenate(
                        [expand(cumc[ci], H + head + 2 * j) for j in range(2)], axis=1
                    )
                    x = xs[s, c * Q : (c + 1) * Q, hcols].astype(F32)
                    inc = dot(bt[ci], (x * fx).astype(BF16))
                    if c > 0:
                        inc = inc + sl[s, c - 1, :, hcols] * rowx[ci : ci + 1, hcols]
                    if c + 1 < chunks:
                        sl[s, c, :, hcols] = inc
                    else:
                        ends[s, :, at : at + 256] = inc
        parts = [ends[s].reshape(N // 8, 8, GC) for s in range(series_here)]
        isend[g] = jnp.concatenate(parts, axis=1).astype(BF16)

        if g == 0:
            to_peers(lambda k: dsend, drecv, d_ssem.at[0], d_rsem.at[0])
            drecv[me] = dsend[...]
        to_peers(lambda k: isend.at[g, k], irecv.at[g], i_ssem.at[g], i_rsem.at[g])
        irecv[g, me] = isend[g, me]

    def server(g):
        col0 = g * GC
        if g == 0:
            d_all.wait_recv()
        dall = jnp.exp2(drecv[...].reshape(n_tm * 8, 128))
        for j in range(GC // 128):
            wide = expand(dall, (col0 + j * 128) // 64)
            dxs[:, :, j * 128 : (j + 1) * 128] = wide.reshape(n_tm, 8, 128)

        i_all[g].wait_recv()
        s0 = s1 = jnp.zeros((8, GC), F32)
        for k in range(n_tm):
            ssend[g, k] = jnp.concatenate([s0, s1], axis=0).astype(BF16)
            if k + 1 < n_tm:
                part = irecv[g, k].astype(F32)
                s0 = s0 * dxs[k, 0:1, :] + part[0:8]
                s1 = s1 * dxs[k, 1:2, :] + part[8:16]
        srecv[g, me] = ssend[g, me]
        to_peers(lambda k: ssend.at[g, k], srecv.at[g], s_ssem.at[g], s_rsem.at[g])

    lanes1 = lax.broadcasted_iota(jnp.int32, (1, 128), 1)
    left = jnp.where(lanes1 < 64, 1.0, 0.0).astype(BF16)
    right = jnp.where(lanes1 < 64, 0.0, 1.0).astype(BF16)

    def intra(lo, hi):
        def intra_chunk(ci):
            s = ci // chunks
            t0 = pl.multiple_of((ci % chunks) * Q, 16)
            r0 = pl.multiple_of(ci * Q, 16)
            for p in range(H // 2):
                ws = []
                for h in (2 * p, 2 * p + 1):
                    d = cumc[ci, :, h : h + 1] - crt[ci, h : h + 1, :]
                    ws.append((jnp.exp2(jnp.minimum(d, 100.0)) * scs[ci]).astype(BF16))
                xp = xs[s, pl.ds(t0, Q), p * 128 : (p + 1) * 128]
                rhs = jnp.concatenate([xp * left, xp * right], axis=0)
                y = dot(jnp.concatenate(ws, axis=1), rhs)
                y = y + xp.astype(F32) * rowx[16:17, p * 128 : (p + 1) * 128]
                yb[pl.ds(r0, Q), p * 128 : (p + 1) * 128] = y

        def intra_body(i, carry):
            for half in range(2):
                g0 = pl.multiple_of((2 * i + half) * 256, 256)
                h = dot(tok[1, RIM:, :], wgate[:, pl.ds(g0, 256)]) * 0.5
                sg[steps : 2 * steps, pl.ds(g0, 256)] = h + h * jnp.tanh(h)
                intra_chunk(2 * i + half)
            return carry

        lax.fori_loop(lo, hi, intra_body, 0)

    scoped("group0", group, 0)
    scoped("group1", group, 1)
    scoped("group2", group, 2)
    scoped("server0", server, 0)
    scoped("group3", group, 3)
    scoped("server1", server, 1)
    scoped("intra0", intra, 0, nc // 4)
    scoped("server2", server, 2)
    scoped("intra1", intra, nc // 4, nc // 2)
    scoped("server3", server, 3)
    loads[3].wait()

    def arrive(g):
        s_all[g].wait_recv()
        got = srecv[g].astype(F32)
        for s in range(series_here):
            sin[s] = got[:, 8 * s : 8 * s + 8, :].reshape(N, GC)

    def mix(g, s, c):
        ci = s * chunks + c
        r = slice(ci * Q, (ci + 1) * Q)
        cc = xs[s, c * Q : (c + 1) * Q, DI + N : DI + 2 * N]
        total = None if g == 0 else ssq[r, :]
        for half in range(2):
            at = half * 256
            cols = slice(g * GC + at, g * GC + at + 256)
            st = sin[s, :, at : at + 256]
            if c > 0:
                st = st * rowx[8 + ci : 9 + ci, cols] + sl[s, c - 1, :, cols]
            inter = dot(cc, st.astype(BF16))
            gx = dot(ghl[ci], eh[:, cols])
            gated = (yb[r, cols] + gx * inter) * sg[r, cols]
            gain = gain_ref[cols].reshape(1, 256)
            nbs[s][c * Q : (c + 1) * Q, at : at + 256] = (gated * gain).astype(BF16)
            sq = gated * gated
            for j in range(2):
                piece = sq[:, j * 128 : (j + 1) * 128]
                total = piece if total is None else total + piece
        ssq[r, :] = total

    def row_scale(s):
        rs = slice(s * steps, (s + 1) * steps)
        mean = jnp.sum(ssq[rs, :], axis=1, keepdims=True) * (1.0 / DI)
        scale = lax.rsqrt(mean + EPS)
        for c in range(chunks):
            live = jnp.where(lenv[s] > (me * steps + c * Q).astype(F32), 1.0, 0.0)[0:1, 0:1]
            piece = scale[c * Q : (c + 1) * Q] * live
            ssq[s * steps + c * Q : s * steps + (c + 1) * Q, :] = jnp.broadcast_to(piece, (Q, 128))

    def leave(g, s, n):
        acc = raw_a if n < 2 else raw_b
        at = (n % 2) * 2
        part = dot(nbs[s][...], wout[g * GC : (g + 1) * GC, n * 256 : (n + 1) * 256])
        for j in range(2):
            piece = part[:, j * 128 : (j + 1) * 128]
            if g > 0:
                piece = piece + acc[s, at + j, 0:steps, :]
            if g < GROUPS - 1:
                acc[s, at + j, 0:steps, :] = piece
            else:
                lo = n * 256 + j * 128
                res = piece * ssq[s * steps : (s + 1) * steps, :]
                out_ref[s, :, lo : lo + 128] = res.astype(BF16)

    for g in range(GROUPS):
        if g == GROUPS - 1:
            for c in range(chunks):
                leave(g - 1, 1, c)
        scoped("arrive", arrive, g)
        with jax.named_scope("final"):
            for c in range(chunks):
                mix(g, 0, c)
                if 0 < g < GROUPS - 1:
                    leave(g - 1, 1, c)
            if g == GROUPS - 1:
                row_scale(0)
            for c in range(chunks):
                mix(g, 1, c)
                leave(g, 0, c)
    with jax.named_scope("last"):
        row_scale(1)
        for c in range(chunks):
            leave(GROUPS - 1, 1, c)

    len_all().wait_send()

    @pl.when(me < n_tm - 1)
    def _():
        for s in range(series_here):
            rim_copy(s).wait_send()

    d_all.wait_send()
    for g in range(GROUPS):
        i_all[g].wait_send()
        s_all[g].wait_send()


def body(
    n_tm,
    n_ser,
    tokens,
    gate_proj,
    input_proj,
    step_proj,
    conv_kernel,
    conv_bias,
    step_bias,
    decay_rate,
    skip_gain,
    norm_gain,
    out_proj,
    lengths,
    slot_series,
):
    series_here, steps, _ = tokens.shape
    chunks = steps // Q
    nc = series_here * chunks
    any_spec = pl.BlockSpec(memory_space=pl.ANY)
    vmem = pl.BlockSpec(memory_space=pltpu.VMEM)
    smem = pl.BlockSpec(memory_space=pltpu.SMEM)
    dma = pltpu.SemaphoreType.DMA
    scratch = [
        pltpu.VMEM((series_here, RIM + steps, D), BF16),
        pltpu.VMEM((D, W_IN), BF16),
        pltpu.VMEM((D, DI), BF16),
        pltpu.VMEM((DI, D), BF16),
        pltpu.VMEM((series_here, steps, W_IN), BF16),
        pltpu.VMEM((nc, N, Q), BF16),
        pltpu.VMEM((series_here, GC // 128, RIM + steps, 128), F32),
        pltpu.VMEM((series_here, GC // 128, RIM + steps, 128), F32),
        pltpu.VMEM((nc, Q, 128), F32),
        pltpu.VMEM((nc, H, Q), F32),
        pltpu.VMEM((nc, Q, Q), F32),
        pltpu.VMEM((nc * H, Q), F32),
        pltpu.VMEM((24, 128), F32),
        pltpu.VMEM((24, DI), F32),
        pltpu.VMEM((series_here, chunks - 1, N, DI), F32),
        pltpu.VMEM((series_here, N, GC), F32),
        pltpu.VMEM((series_here, N, GC), F32),
        pltpu.VMEM((series_here * steps, 128), F32),
        pltpu.VMEM((nc, Q, 2 * H), BF16),
        pltpu.VMEM((2 * H, DI), BF16),
        pltpu.VMEM((series_here * steps, DI), F32),
        pltpu.VMEM((series_here * steps, DI), F32),
        pltpu.VMEM((steps, GC), BF16),
        pltpu.VMEM((steps, GC), BF16),
        pltpu.VMEM((GROUPS, n_tm, 16, GC), BF16),
        pltpu.VMEM((GROUPS, n_tm, 16, GC), BF16),
        pltpu.VMEM((GROUPS, n_tm, 16, GC), BF16),
        pltpu.VMEM((GROUPS, n_tm, 16, GC), BF16),
        pltpu.VMEM((8, 128), F32),
        pltpu.VMEM((n_tm, 8, 128), F32),
        pltpu.VMEM((n_tm, 8, GC), F32),
        pltpu.VMEM((8, 128), jnp.int32),
        pltpu.VMEM((n_ser, 8, 128), jnp.int32),
        pltpu.VMEM((series_here, 8, 128), F32),
        dma((4 + GATE_PIECES,)),
        dma((1,)),
        dma((1,)),
        dma((series_here,)),
        dma((series_here,)),
        dma((1,)),
        dma((1,)),
        dma((GROUPS,)),
        dma((GROUPS,)),
        dma((GROUPS,)),
        dma((GROUPS,)),
    ]
    return pl.pallas_call(
        functools.partial(kernel, n_tm, n_ser, series_here, steps),
        out_shape=pltpu.VMEM(tokens.shape, BF16),
        in_specs=[any_spec] * 3 + [vmem] * 7 + [any_spec] + [smem] * 2,
        out_specs=vmem,
        scratch_shapes=scratch,
        compiler_params=pltpu.CompilerParams(
            collective_id=0,
            has_side_effects=True,
            vmem_limit_bytes=VMEM,
        ),
        name="mixer",
    )(
        tokens,
        gate_proj,
        input_proj,
        step_proj.T,
        conv_kernel,
        conv_bias,
        step_bias,
        decay_rate,
        skip_gain,
        norm_gain,
        out_proj,
        lengths,
        slot_series,
    )


def solution(mesh):
    n_tm, n_ser = mesh.shape["tm"], mesh.shape["series"]
    in_specs = (P("series", "tm", None),) + (P(),) * 10 + (P("series"), P("series"))
    return jax.shard_map(
        functools.partial(body, n_tm, n_ser),
        mesh=mesh,
        in_specs=in_specs,
        out_specs=P("series", "tm", None),
        check_vma=False,
    )
```
